32 devices in a mesh: groups: 2 (over y), wide: 4 (over x, core), tp: 4 (over z).
Axes of the slice: x: 2, y: 2, z: 4, core: 2. Of those that a mesh axis runs over, the one named last changes fastest.
Arguments:
- patches: bfloat16 [2048, 1280], P(('groups', 'wide')), parts along dimension 0, may hold values from -190 to 190
- patch_counts: int32 [64], P('groups'), parts along dimension 0, may hold values from 24 to 32, as said below
- placement: int32 [64, 2], P('groups'), parts along dimension 0, may hold values from 0 to 511, as said below
- positions: int32 [3, 4096], P(None, ('groups', 'wide')), parts along dimension 1, may hold values from 0 to 2047
- text_embeds: bfloat16 [4096, 8192], P(('groups', 'wide'), 'tp'), parts along dimension 0, may hold values from -180 to 180
- vit_gain: float32 [1280], replicated, may hold values from 0.1 to 1.9
- vit_qkv: bfloat16 [1280, 3, 1280], P(None, None, 'tp'), may hold values from -4 to 4
- vit_proj: bfloat16 [1280, 1280], P('tp'), may hold values from -0.15625 to 0.15625
- merger_gain: float32 [1280], replicated, may hold values from 0.1 to 1.9
- merger_up: bfloat16 [5120, 2560], P(None, 'tp'), may hold values from -0.078125 to 0.078125
- merger_down: bfloat16 [2560, 8192], P('tp'), may hold values from -0.15625 to 0.15625
- llm_gain: float32 [8192], replicated, may hold values from 0.1 to 1.9
- llm_query: bfloat16 [8192, 4096], P('wide', 'tp'), may hold values from -0.0625 to 0.0625
- llm_key: bfloat16 [8192, 1024], P('wide', 'tp'), may hold values from -0.0625 to 0.0625
- llm_value: bfloat16 [8192, 1024], P('wide', 'tp'), may hold values from -0.0625 to 0.0625
Outputs:
- query: bfloat16 [4096, 4096], P(('groups', 'wide'), 'tp'), parts along dimension 0
- key_cache: bfloat16 [4096, 1024], P(('groups', 'wide'), 'tp'), parts along dimension 0
- value_cache: bfloat16 [4096, 1024], P(('groups', 'wide'), 'tp'), parts along dimension 0
The draws below stay inside these ranges and needn't reach their ends.
There are 2 independent parts, one for each index of `groups`. The reference program is written for one: setup_inputs(seed, part) draws one part's arguments, and reference() takes and returns one part's arrays. A program takes and returns all parts, laid end to end along the dimension named above; an argument that names none is the same for every part. Nothing has to cross between parts.
Inputs may be any that keep to these rules, and one draw needn't show every extreme that they name: `patch_counts`: each count is a multiple of 4; images 8 * s to 8 * s + 7 belong to encoder device s of the wide axis; patch rows 4 m to 4 m + 3 of an image form its merged row m. `placement`: column 0 is the owner on the wide axis, column 1 the first of the image's merged rows among that owner's 512 rows. Images' merged rows never intersect and stay within the owner's rows. Each owner receives 8 images. At most 16 merged rows go from one encoder device to one owner, and that number is reached in every draw.
All inputs are finite; a program needn't handle non-finite values.
Results may differ from the reference program's by a relative error of at most 0.015.
Values may be sent and summed in bfloat16 or wider, within the bound.
A program may use at most 128 MiB of HBM per device.

```python
import jax
import jax.numpy as jnp
from jax import lax

VD = 1280
VH = 16
LD = 8192
KVH = 8
HD = 128
QH = 32
MH = 2560
IMG_DEV = 8
MAXP = 32
TOK_DEV = 512
VHD = 80
MAXM = 8
IMAGES = 32
TOKENS = 2048
N_TP = 4


def layout_tables(key):
    width_wide = IMAGES // IMG_DEV
    rank_key, owner_key, count_key, shift_key = jax.random.split(jax.random.fold_in(key, 7), 4)
    source_rank = jax.random.permutation(rank_key, width_wide).astype(jnp.int32)
    owner_order = jax.random.permutation(owner_key, width_wide).astype(jnp.int32)
    image_ids = jnp.arange(IMAGES, dtype=jnp.int32)
    source = image_ids // IMG_DEV
    within = image_ids % IMG_DEV
    owner_ids = owner_order[(source_rank[source] + within) % width_wide]
    lowest = max(1, 3 * MAXM // 4)
    merged = jax.random.randint(count_key, (IMAGES,), lowest, MAXM + 1).astype(jnp.int32)
    forced = (source == 0) & (within % width_wide == 0)
    merged = jnp.where(forced, MAXM, merged).astype(jnp.int32)
    slot_rows = TOK_DEV // IMG_DEV
    shift_rows = jax.random.randint(shift_key, (IMAGES,), 0, slot_rows - merged + 1).astype(jnp.int32)
    start_rows = within * slot_rows + shift_rows
    return (merged * 4, jnp.stack([owner_ids, start_rows], axis=1))


def draw_patch_counts(key, part):
    return layout_tables(key)[0].astype(jnp.int32)


def draw_placement(key, part):
    return layout_tables(key)[1].astype(jnp.int32)


def draw_patches(key, part):
    base_key = jax.random.fold_in(jax.random.fold_in(key, 13), 0)
    total_rows = IMAGES * MAXP
    field = jnp.clip(jax.random.normal(base_key, (total_rows, VD), jnp.float32), -4.0, 4.0)
    return field.astype(jnp.bfloat16)


def draw_text_embeds(key, part):
    base_key = jax.random.fold_in(jax.random.fold_in(key, 17), 0)
    field = jnp.clip(jax.random.normal(base_key, (TOKENS, LD), jnp.float32), -4.0, 4.0)
    return field.astype(jnp.bfloat16)


def draw_vit_qkv(key, part):
    base_key = jax.random.fold_in(jax.random.fold_in(key, 11), 0)
    base = jnp.clip(jax.random.normal(base_key, (VD, 3, VD), jnp.float32), -4.0, 4.0) * VD ** (-0.5)
    return base.astype(jnp.bfloat16)


def plant(drawn, rng, low, top_value):
    place = [jax.random.randint(jax.random.fold_in(rng, axis), (), 0, length) for axis, length in enumerate(drawn.shape)]
    widest = drawn.shape.index(max(drawn.shape))
    beside = place[:widest] + [(place[widest] + 1) % drawn.shape[widest]] + place[widest + 1:]
    return drawn.at[tuple(place)].set(low).at[tuple(beside)].set(top_value)


def spiked(result, rng, source, target, parts, factor):
    owner, partner = [(jnp.arange(result.shape[dim]) // (result.shape[dim] // parts)).reshape([-1 if axis == dim else 1 for axis in range(result.ndim)]) for dim in (source, target)]
    chosen = jax.random.permutation(rng, parts)[partner]
    strong = (owner == chosen) | (owner == (partner + parts // 2) % parts)
    return jnp.where(strong, factor * result, result)


def block_levels(stream_key, extent, shards, least, high):
    def one(dim, blocks):
        draws = jax.random.uniform(jax.random.fold_in(jax.random.fold_in(stream_key, 6), dim), (blocks,), jnp.float32, least / len(shards), high / len(shards))
        return jnp.repeat(jnp.exp(draws), extent[dim] // blocks).reshape((-1,) + (1,) * (len(extent) - dim - 1))

    gain = one(*shards[0])
    for cut in shards[1:]:
        gain = gain * one(*cut)
    return gain


def bell_draw(key, extent, scale, most, cuts=(), kind=jnp.bfloat16):
    drawn = scale * jax.random.normal(key, extent, jnp.float32)
    if cuts:
        drawn = drawn * block_levels(key, extent, cuts, -0.22, 0.18)
    return jnp.clip(drawn, -most, most).astype(kind)


def heavy_noise(own_key, dims, scale, bound, shards, heavy, kind=jnp.bfloat16):
    array = scale * jax.random.normal(own_key, dims, jnp.float32)
    if shards:
        array = array * block_levels(own_key, dims, shards, -0.22, 0.18)
    return jnp.clip(spiked(array, jax.random.fold_in(own_key, 3), *heavy), -bound, bound).astype(kind)


def setup_inputs(seed: int = 0, part: int = 0) -> dict:
    keys = jax.random.split(jax.random.key(seed), 16)
    part_splits = jax.random.split(jax.random.fold_in(keys[15], part), 16)
    return {
        "patches": draw_patches(jax.random.fold_in(jax.random.fold_in(keys[15], part), 71), part),
        "patch_counts": draw_patch_counts(jax.random.fold_in(jax.random.fold_in(keys[15], part), 71), part),
        "placement": draw_placement(jax.random.fold_in(jax.random.fold_in(keys[15], part), 71), part),
        "positions": plant(jax.random.randint(part_splits[3], (3, TOKENS), 0, TOKENS), jax.random.fold_in(part_splits[3], 1), 0, TOKENS - 1).astype(jnp.int32),
        "text_embeds": draw_text_embeds(jax.random.fold_in(jax.random.fold_in(keys[15], part), 71), part),
        "vit_gain": jnp.clip(1.0 + 0.18 * jax.random.normal(keys[5], (VD,), jnp.float32), 0.1, 1.9),
        "vit_qkv": draw_vit_qkv(jax.random.fold_in(keys[15], 71), part),
        "vit_proj": bell_draw(keys[7], (VD, VD), VD ** -0.5, 0.15625, ((0, 4),)),
        "merger_gain": jnp.clip(1.0 + 0.18 * jax.random.normal(keys[8], (VD,), jnp.float32), 0.1, 1.9),
        "merger_up": bell_draw(keys[9], (4 * VD, MH), (4 * VD) ** -0.5, 0.078125, ((1, 4),)),
        "merger_down": heavy_noise(keys[10], (MH, LD), MH ** -0.5, 0.15625, ((0, 4),), (0, 1, 4, 2.0)),
        "llm_gain": jnp.clip(1.0 + 0.18 * jax.random.normal(keys[11], (LD,), jnp.float32), 0.1, 1.9),
        "llm_query": bell_draw(keys[12], (LD, QH * HD), LD ** -0.5, 0.0625, ((0, 4), (1, 4))),
        "llm_key": bell_draw(keys[13], (LD, KVH * HD), LD ** -0.5, 0.0625, ((0, 4), (1, 4))),
        "llm_value": bell_draw(keys[14], (LD, KVH * HD), LD ** -0.5, 0.0625, ((0, 4), (1, 4))),
    }


NORM_EPS = 1e-06
ROPE_BASE = 1000000.0

def layer_norm(inputs, scale_gain):
    center = lax.optimization_barrier(jnp.mean(inputs, axis=-1, keepdims=True))
    shifted = inputs - center
    spread = lax.optimization_barrier(jnp.mean(shifted * shifted, axis=-1, keepdims=True))
    return shifted * lax.rsqrt(spread + NORM_EPS) * scale_gain

def rms_norm(inputs, scale_gain):
    square = lax.optimization_barrier(jnp.mean(inputs * inputs, axis=-1, keepdims=True))
    return inputs * lax.rsqrt(square + NORM_EPS) * scale_gain

def rotary(values, positions):
    half_size = HD // 2
    frequency = jnp.arange(half_size).astype(jnp.float32)
    inverse = ROPE_BASE ** (-2.0 * frequency / HD)
    first_end = HD // 8
    second = first_end + 3 * HD // 16
    ordinal = jnp.arange(half_size)
    section = jnp.where(ordinal < first_end, 0, jnp.where(ordinal < second, 1, 2))
    chosen = jnp.where(section[:, None] == 0, positions[0][None, :], jnp.where(section[:, None] == 1, positions[1][None, :], positions[2][None, :]))
    angles = chosen.T.astype(jnp.float32) * inverse[None, :]
    angles = jnp.concatenate([angles, angles], axis=1)
    cosine = jnp.cos(angles)[:, None, :]
    sine_table = jnp.sin(angles)[:, None, :]
    upper_half = values[..., :half_size]
    lower_half = values[..., half_size:]
    turned = jnp.concatenate([-lower_half, upper_half], axis=-1)
    return values * cosine + turned * sine_table

def reference(patches, patch_counts, placement, positions, text_embeds, vit_gain, vit_qkv, vit_proj, merger_gain, merger_up, merger_down, llm_gain, llm_query, llm_key, llm_value):
    patch_rows = patches.astype(jnp.float32)
    normed = layer_norm(patch_rows, vit_gain).astype(jnp.bfloat16)
    triple = jnp.dot(normed, vit_qkv.reshape(VD, 3 * VD), preferred_element_type=jnp.float32)
    triple = lax.optimization_barrier(triple.astype(jnp.bfloat16))
    triple = triple.reshape(IMAGES, MAXP, 3, VH, VHD).astype(jnp.float32)
    scores = jnp.einsum('iqhd,ikhd->ihqk', triple[:, :, 0], triple[:, :, 1]) * VHD ** (-0.5)
    present = jnp.arange(MAXP)[None, :] < patch_counts[:, None]
    scores = jnp.where(present[:, None, None, :], scores, -jnp.inf)
    highest = lax.optimization_barrier(jnp.max(scores, axis=-1, keepdims=True))
    raised = jnp.exp(scores - highest)
    attention_weights = (raised / lax.optimization_barrier(jnp.sum(raised, axis=-1, keepdims=True))).astype(jnp.bfloat16)
    attention_weights = lax.optimization_barrier(attention_weights).astype(jnp.float32)
    context = jnp.einsum('ihqk,ikhd->iqhd', attention_weights, triple[:, :, 2])
    context = context.astype(jnp.bfloat16).reshape(IMAGES * MAXP, VD)
    group_width = VD // N_TP
    attended = jnp.zeros((IMAGES * MAXP, VD), jnp.float32)
    for member in range(N_TP):
        share = jnp.dot(context[:, member * group_width:(member + 1) * group_width], vit_proj[member * group_width:(member + 1) * group_width], preferred_element_type=jnp.float32)
        attended = attended + lax.optimization_barrier(share.astype(jnp.bfloat16)).astype(jnp.float32)
    mixed_rows = patch_rows + attended
    merged_in = layer_norm(mixed_rows, merger_gain).astype(jnp.bfloat16).reshape(IMAGES * MAXM, 4 * VD)
    hidden = jax.nn.gelu(jnp.dot(merged_in, merger_up, preferred_element_type=jnp.float32), approximate=False).astype(jnp.bfloat16)
    unit_width = MH // N_TP
    summed = jnp.zeros((IMAGES * MAXM, LD), jnp.float32)
    for member in range(N_TP):
        share = jnp.dot(hidden[:, member * unit_width:(member + 1) * unit_width], merger_down[member * unit_width:(member + 1) * unit_width], preferred_element_type=jnp.float32)
        summed = summed + lax.optimization_barrier(share.astype(jnp.bfloat16)).astype(jnp.float32)
    visual = summed.astype(jnp.bfloat16)
    merged_count = patch_counts // 4
    offsets = jnp.arange(MAXM).astype(jnp.int32)
    targets = placement[:, 0:1] * TOK_DEV + placement[:, 1:2] + offsets[None, :]
    targets = jnp.where(offsets[None, :] < merged_count[:, None], targets, TOKENS).astype(jnp.int32)
    prompt_rows = text_embeds.at[targets.reshape(-1)].set(visual, mode='drop')
    normed_prompt = rms_norm(prompt_rows.astype(jnp.float32), llm_gain).astype(jnp.bfloat16)
    queries = jnp.dot(normed_prompt, llm_query, preferred_element_type=jnp.float32).reshape(TOKENS, QH, HD)
    queries = rotary(queries, positions).astype(jnp.bfloat16).reshape(TOKENS, QH * HD)
    key_rows = jnp.dot(normed_prompt, llm_key, preferred_element_type=jnp.float32).reshape(TOKENS, KVH, HD)
    key_rows = rotary(key_rows, positions).astype(jnp.bfloat16).reshape(TOKENS, KVH * HD)
    value_rows = jnp.dot(normed_prompt, llm_value, preferred_element_type=jnp.float32).astype(jnp.bfloat16)
    return (queries, key_rows, value_rows)
```

```python
import functools

import jax
import jax.numpy as jnp
from jax import lax
from jax.experimental import pallas as pl
from jax.experimental.pallas import tpu as pltpu
from jax.sharding import PartitionSpec as P

VD = 1280
HD = 128
IMG_DEV = 8
MAXP = 32
TOK_DEV = 512
VHD = 80
MAXM = 8


NORM_EPS = 1e-06
ROPE_BASE = 1000000.0


def layer_norm(inputs, scale_gain):
    center = jnp.mean(inputs, axis=-1, keepdims=True)
    shifted = inputs - center
    spread = jnp.mean(shifted * shifted, axis=-1, keepdims=True)
    return shifted * lax.rsqrt(spread + NORM_EPS) * scale_gain


def rms_norm(inputs, scale_gain):
    square = jnp.mean(inputs * inputs, axis=-1, keepdims=True)
    return inputs * lax.rsqrt(square + NORM_EPS) * scale_gain


def rotary(values, positions):
    half_size = HD // 2
    frequency = jnp.arange(half_size).astype(jnp.float32)
    inverse = ROPE_BASE ** (-2.0 * frequency / HD)
    first_end = HD // 8
    second = first_end + 3 * HD // 16
    ordinal = jnp.arange(half_size)
    section = jnp.where(ordinal < first_end, 0, jnp.where(ordinal < second, 1, 2))
    chosen = jnp.where(
        section[:, None] == 0,
        positions[0][None, :],
        jnp.where(section[:, None] == 1, positions[1][None, :], positions[2][None, :]),
    )
    angles = chosen.T.astype(jnp.float32) * inverse[None, :]
    angles = jnp.concatenate([angles, angles], axis=1)
    cosine = jnp.cos(angles)[:, None, :]
    sine_table = jnp.sin(angles)[:, None, :]
    upper_half = values[..., :half_size]
    lower_half = values[..., half_size:]
    turned = jnp.concatenate([-lower_half, upper_half], axis=-1)
    return values * cosine + turned * sine_table


def handoff_tables(patch_counts, placement, width_wide, myself, capacity):
    merged_count = patch_counts // 4
    owners = placement[:, 0]
    starts = placement[:, 1]
    owner_grid = owners.reshape(width_wide, IMG_DEV)
    count_grid = merged_count.reshape(width_wide, IMG_DEV)
    ordinal = jnp.arange(IMG_DEV)
    before = ordinal[:, None] < ordinal[None, :]
    same_owner = owner_grid[:, :, None] == owner_grid[:, None, :]
    offsets = jnp.sum(jnp.where(same_owner & before[None], count_grid[:, :, None], 0), axis=1)
    mine_owner = lax.dynamic_index_in_dim(owner_grid, myself, 0, keepdims=False)
    mine_count = lax.dynamic_index_in_dim(count_grid, myself, 0, keepdims=False)
    mine_offset = lax.dynamic_index_in_dim(offsets, myself, 0, keepdims=False)
    target = jnp.arange(width_wide)[:, None, None]
    slot_index = jnp.arange(capacity)[None, :, None]
    matches = (
        (mine_owner[None, None, :] == target)
        & (slot_index >= mine_offset[None, None, :])
        & (slot_index < mine_offset[None, None, :] + mine_count[None, None, :])
    )
    source_row = ordinal[None, None, :] * MAXM + slot_index - mine_offset[None, None, :]
    send_index = jnp.sum(jnp.where(matches, source_row, 0), axis=-1)
    send_live = jnp.any(matches, axis=-1)
    row_place = jnp.arange(TOK_DEV)[:, None]
    inside = (
        (owners[None, :] == myself)
        & (row_place >= starts[None, :])
        & (row_place < starts[None, :] + merged_count[None, :])
    )
    image_source = jnp.arange(owners.shape[0]) // IMG_DEV
    flat_slot = (
        image_source[None, :] * capacity
        + offsets.reshape(-1)[None, :]
        + row_place
        - starts[None, :]
    )
    take_index = jnp.sum(jnp.where(inside, flat_slot, 0), axis=-1)
    take_live = jnp.any(inside, axis=-1)
    return (send_index, send_live, take_index, take_live)


def pack_rows(visual, send_index, send_live):
    picked = jnp.take(visual, send_index.reshape(-1), axis=0)
    picked = picked.reshape(send_index.shape + (visual.shape[1],))
    return jnp.where(send_live[..., None], picked, jnp.zeros((), visual.dtype))


def exchange_sum(partial, axis_name, split_axis):
    members = lax.axis_size(axis_name)
    shape = partial.shape
    cut = shape[:split_axis] + (members, shape[split_axis] // members) + shape[split_axis + 1 :]
    stacked = jnp.moveaxis(partial.reshape(cut), split_axis, 0)
    swapped = lax.all_to_all(stacked, axis_name, split_axis=0, concat_axis=0, tiled=True)
    return jnp.sum(swapped.astype(jnp.float32), axis=0)


def doubling_gather(block, axis_name):
    members = lax.axis_size(axis_name)
    held = {0: block}
    bits = []
    step = 1
    while step < members:
        bits.append(step)
        step *= 2
    for bit in bits[1:] + bits[:1]:
        pairs = [(source, source ^ bit) for source in range(members)]
        for entry in sorted(held):
            held[entry ^ bit] = lax.ppermute(held[entry], axis_name, pairs)
    return [held[entry] for entry in range(members)]


def ring_gather_columns(block, axis_name):
    members = lax.axis_size(axis_name)
    me = lax.axis_index(axis_name)
    width = block.shape[1]
    up = [(source, (source + 1) % members) for source in range(members)]
    down = [(source, (source - 1) % members) for source in range(members)]
    gathered = jnp.zeros((block.shape[0], width * members), block.dtype)
    pieces = [(0, 0, block)]
    forward, backward = block, block
    distance = 1
    while 2 * distance < members:
        forward = lax.ppermute(forward, axis_name, up)
        backward = lax.ppermute(backward, axis_name, down)
        pieces.append((members - distance, 0, forward))
        pieces.append((distance, 0, backward))
        distance += 1
    if 2 * distance == members:
        half = width // 2
        pieces.append((distance, 0, lax.ppermute(forward[:, :half], axis_name, up)))
        pieces.append((distance, half, lax.ppermute(backward[:, half:], axis_name, down)))
    for offset, inner, piece in pieces:
        column = lax.rem(me + offset, members) * width + inner
        gathered = lax.dynamic_update_slice(gathered, piece, (0, column))
    return gathered


def project(rows, weight_blocks, member):
    depth = weight_blocks[0].shape[0]
    total = None
    for entry, block in enumerate(weight_blocks):
        columns = lax.dynamic_slice_in_dim(rows, (member ^ entry) * depth, depth, 1)
        share = jnp.dot(columns, block, preferred_element_type=jnp.float32)
        total = share if total is None else total + share
    return total


def per_device_rings(
    patches,
    patch_counts,
    placement,
    positions,
    text_embeds,
    vit_gain,
    vit_qkv,
    vit_proj,
    merger_gain,
    merger_up,
    merger_down,
    llm_gain,
    llm_query,
    llm_key,
    llm_value,
):
    width_wide = lax.axis_size("wide")
    myself = lax.axis_index("wide")
    capacity = MAXM * ((IMG_DEV + width_wide - 1) // width_wide)
    local_heads = vit_qkv.shape[2] // VHD
    own_weights = jnp.concatenate([llm_query, llm_key, llm_value], axis=1)
    weight_blocks = doubling_gather(own_weights, "wide")
    text_rows = ring_gather_columns(text_embeds, "tp")
    members = lax.axis_size("tp")
    patch_rows = patches.astype(jnp.float32)
    normed = layer_norm(patch_rows, vit_gain).astype(jnp.bfloat16)
    triple = jnp.dot(normed, vit_qkv.reshape(VD, -1), preferred_element_type=jnp.float32).astype(
        jnp.bfloat16
    )
    triple = triple.reshape(IMG_DEV, MAXP, 3, local_heads, VHD)
    scores = jnp.einsum(
        "iqhd,ikhd->ihqk", triple[:, :, 0], triple[:, :, 1], preferred_element_type=jnp.float32
    ) * VHD ** (-0.5)
    own_counts = lax.dynamic_slice_in_dim(patch_counts, myself * IMG_DEV, IMG_DEV)
    present = jnp.arange(MAXP)[None, :] < own_counts[:, None]
    scores = jnp.where(present[:, None, None, :], scores, -jnp.inf)
    highest = jnp.max(scores, axis=-1, keepdims=True)
    raised = jnp.exp(scores - highest)
    attention_weights = (raised / jnp.sum(raised, axis=-1, keepdims=True)).astype(jnp.bfloat16)
    context = jnp.einsum(
        "ihqk,ikhd->iqhd", attention_weights, triple[:, :, 2], preferred_element_type=jnp.float32
    ).astype(jnp.bfloat16)
    context = context.reshape(IMG_DEV * MAXP, local_heads * VHD)
    partial_heads = jnp.dot(context, vit_proj, preferred_element_type=jnp.float32)
    attended = exchange_sum(partial_heads.astype(jnp.bfloat16), "tp", 0)
    own_rows = IMG_DEV * MAXP // members
    own_patches = lax.dynamic_slice_in_dim(patches, lax.axis_index("tp") * own_rows, own_rows, 0)
    mixed_rows = own_patches.astype(jnp.float32) + attended
    own_merged = layer_norm(mixed_rows, merger_gain).astype(jnp.bfloat16)
    own_merged = own_merged.reshape(own_rows * MAXM // MAXP, 4 * VD)
    merged_in = lax.all_gather(own_merged, "tp", axis=0, tiled=True)
    hidden = jax.nn.gelu(
        jnp.dot(merged_in, merger_up, preferred_element_type=jnp.float32), approximate=False
    ).astype(jnp.bfloat16)
    partial_visual = jnp.dot(hidden, merger_down, preferred_element_type=jnp.float32)
    send_index, send_live, take_index, take_live = handoff_tables(
        patch_counts, placement, width_wide, myself, capacity
    )
    visual = exchange_sum(partial_visual.astype(jnp.bfloat16), "tp", 1).astype(jnp.bfloat16)
    outgoing = pack_rows(visual, send_index, send_live)
    incoming = lax.all_to_all(outgoing, "wide", split_axis=0, concat_axis=0, tiled=True)
    incoming = incoming.reshape(-1, incoming.shape[-1])
    copies = jnp.broadcast_to(incoming[None], (members,) + incoming.shape)
    spread_rows = lax.all_to_all(copies, "tp", split_axis=0, concat_axis=0, tiled=True)
    visual_rows = jnp.swapaxes(spread_rows, 0, 1).reshape(incoming.shape[0], -1)
    normed_text = rms_norm(text_rows.astype(jnp.float32), llm_gain).astype(jnp.bfloat16)
    normed_visual = rms_norm(visual_rows.astype(jnp.float32), llm_gain).astype(jnp.bfloat16)
    projected_text = project(normed_text, weight_blocks, myself)
    projected_visual = project(normed_visual, weight_blocks, myself)
    placed = jnp.take(projected_visual, take_index, axis=0)
    projected = jnp.where(take_live[:, None], placed, projected_text)
    first = llm_query.shape[1]
    second = first + llm_key.shape[1]
    projected_query = projected[:, :first]
    projected_key = projected[:, first:second]
    projected_value = projected[:, second:]
    queries = (
        rotary(projected_query.reshape(TOK_DEV, -1, HD), positions)
        .astype(jnp.bfloat16)
        .reshape(TOK_DEV, -1)
    )
    key_rows = (
        rotary(projected_key.reshape(TOK_DEV, -1, HD), positions)
        .astype(jnp.bfloat16)
        .reshape(TOK_DEV, -1)
    )
    value_rows = projected_value.astype(jnp.bfloat16)
    return (queries, key_rows, value_rows)


STEPS = 8
MESH = pl.DeviceIdType.MESH
X_OWN, Y_PASS, CORE_OWN, CORE_X, CORE_Y, LINE = range(6)


def prompt_kernel(
    patch_counts,
    placement,
    inverse,
    positions,
    patches,
    vit_gain,
    vit_qkv,
    vit_proj,
    merger_gain,
    merger_up,
    merger_down,
    text,
    gain,
    w_query,
    w_key,
    w_value,
    rows_out,
    weights,
    texts,
    total,
    squares,
    keep,
    scaled,
    up_held,
    part,
    shares_relay,
    shares_crossed,
    shares_sum,
    shares_in,
    merged,
    hidden,
    visual_part,
    visual_relay,
    visual_crossed,
    visual_sum,
    visual_in,
    packed,
    visuals,
    pick,
    place,
    cosine,
    sine,
    local_sem,
    load_sem,
    bulk_send,
    bulk_recv,
    side_send,
    side_recv,
):
    groups, wide, ring = lax.axis_size("groups"), lax.axis_size("wide"), lax.axis_size("tp")
    g, w, t = lax.axis_index("groups"), lax.axis_index("wide"), lax.axis_index("tp")
    core = w + 1 - 2 * lax.rem(w, 2)
    across = lax.rem(w + 2, wide)
    diagonal = across + 1 - 2 * lax.rem(across, 2)
    other = lax.rem(g + 1, groups)
    above, below = {"tp": lax.rem(t + 1, ring)}, {"tp": lax.rem(t + ring - 1, ring)}
    depth = weights.shape[1] // STEPS
    half = depth // groups
    first, second = w_query.shape[1], w_query.shape[1] + w_key.shape[1]
    line = [lax.rem(t + distance, ring) for distance in range(1, ring)]

    barrier = pltpu.get_barrier_semaphore()
    peers = [{"tp": member} for member in line]
    peers += [{"wide": core}, {"wide": across}, {"wide": diagonal}, {"groups": other}]
    for peer in peers:
        pl.semaphore_signal(barrier, inc=1, device_id=peer, device_id_type=MESH)
    pl.semaphore_wait(barrier, len(peers))

    def remote(source, target, send, recv, peer):
        return pltpu.make_async_remote_copy(
            src_ref=source,
            dst_ref=target,
            send_sem=send,
            recv_sem=recv,
            device_id=peer,
            device_id_type=MESH,
        )

    def in_place(kind, step, ref, peer):
        return remote(ref, ref, bulk_send.at[kind, step], bulk_recv.at[kind, step], peer)

    def rows_of(block, step, offset, count):
        start = pl.multiple_of(step * depth + offset, 16)
        return weights.at[block, pl.ds(start, count)]

    bulk = {
        X_OWN: (lambda s: rows_of(w, s, g * half, half), lambda s: rows_of(across, s, g * half, half), {"wide": across}),
        Y_PASS: (lambda s: rows_of(across, s, g * half, half), lambda s: rows_of(across, s, other * half, half), {"groups": other}),
        CORE_OWN: (lambda s: rows_of(w, s, 0, depth), lambda s: rows_of(core, s, 0, depth), {"wide": core}),
        CORE_X: (lambda s: rows_of(across, s, g * half, half), lambda s: rows_of(diagonal, s, g * half, half), {"wide": core}),
        CORE_Y: (lambda s: rows_of(across, s, other * half, half), lambda s: rows_of(diagonal, s, other * half, half), {"wide": core}),
    }

    def send(kind, step):
        in_place(kind, step, bulk[kind][0](step), bulk[kind][2]).start()

    def sent(kind, step):
        in_place(kind, step, bulk[kind][0](step), bulk[kind][2]).wait_send()

    def received(kind, step):
        in_place(kind, step, bulk[kind][1](step), bulk[kind][2]).wait_recv()

    def weight_loads(step):
        rows = pl.ds(pl.multiple_of(step * depth, depth), depth)
        return [
            pltpu.make_async_copy(
                ref.at[rows], weights.at[w, rows, pl.ds(start, ref.shape[1])], local_sem.at[entry, step]
            )
            for entry, (ref, start) in enumerate(((w_query, 0), (w_key, first), (w_value, second)))
        ]

    def text_load(step):
        columns = pl.ds(pl.multiple_of(step * depth, depth), depth)
        return pltpu.make_async_copy(text.at[:, columns], texts.at[t, step], local_sem.at[3, step])

    def up_copy(hop, step, block):
        return in_place(LINE + hop, step, texts.at[block, step], above)

    def down_copy(hop, step, block):
        return in_place(LINE + ring - 1 + hop, step, texts.at[block, step], below)

    def line_send(hop, step, act=lambda copy: copy.start()):
        @pl.when(t + 1 < ring)
        def _():
            @pl.when(t >= hop)
            def _():
                act(up_copy(hop, step, t - hop))

        @pl.when(t > 0)
        def _():
            @pl.when(t + hop < ring)
            def _():
                act(down_copy(hop, step, t + hop))

    def line_received(hop, step):
        @pl.when(t > hop)
        def _():
            up_copy(hop, step, t - 1 - hop).wait_recv()

        @pl.when(t + 1 + hop < ring)
        def _():
            down_copy(hop, step, t + 1 + hop).wait_recv()

    def line_own(step):
        text_load(step).wait()
        line_send(0, step)

    def line_pass(hop, step):
        line_received(hop - 1, step)
        line_send(hop, step)

    def pass_on(step):
        received(X_OWN, step)
        send(Y_PASS, step)
        send(CORE_X, step)

    def pass_core(step):
        received(Y_PASS, step)
        send(CORE_Y, step)

    near = t + 1 - 2 * lax.rem(t, 2)
    beyond = ring - 1 - t
    half_start = ring // 2 * lax.rem(t // 2 + 1, 2)
    inner_member = lax.rem(t // 2 + t, 2) == 1
    outer_member = jnp.logical_not(inner_member)

    def scatter(slot, pieces, relay, crossed, summed, arrived):
        def copy(entry, source, target, member):
            return remote(source, target, side_send.at[slot + entry], side_recv.at[slot + entry], {"tp": member})

        def hand_in(act=lambda copied: copied.start()):
            @pl.when(outer_member)
            def _():
                for entry in range(2):
                    act(copy(entry, pieces(half_start + entry), relay.at[entry], near))
                act(copy(2, pieces(near), arrived, near))

        def swap():
            @pl.when(outer_member)
            def _():
                crossed[...] = jnp.zeros_like(crossed)

            @pl.when(inner_member)
            def _():
                for entry in range(2):
                    copy(entry, relay.at[entry], relay.at[entry], near).wait_recv()
                    added = relay[entry].astype(jnp.float32) + pieces(half_start + entry)[...].astype(jnp.float32)
                    summed[entry] = added.astype(summed.dtype)
                for entry in range(2):
                    copy(3 + entry, summed.at[entry], crossed.at[entry], beyond).start()

        def hand_back():
            @pl.when(inner_member)
            def _():
                for entry in range(2):
                    copy(3 + entry, crossed.at[entry], crossed.at[entry], beyond).wait_recv()
                added = crossed[lax.rem(near, 2)].astype(jnp.float32) + pieces(near)[...].astype(jnp.float32)
                summed[2] = added.astype(summed.dtype)
                copy(5, summed.at[2], arrived, near).start()

        def result():
            @pl.when(inner_member)
            def _():
                copy(2, arrived, arrived, near).wait_recv()

            @pl.when(outer_member)
            def _():
                copy(5, arrived, arrived, near).wait_recv()

            own = pieces(t)[...].astype(jnp.float32)
            return own + arrived[...].astype(jnp.float32) + crossed[lax.rem(t, 2)].astype(jnp.float32)

        def finish():
            hand_in(lambda copied: copied.wait_send())

            @pl.when(inner_member)
            def _():
                for entry in range(2):
                    copy(3 + entry, summed.at[entry], crossed.at[entry], beyond).wait_send()
                copy(5, summed.at[2], arrived, near).wait_send()

        return hand_in, swap, hand_back, result, finish

    def gather(slot, block):
        def copy(distance, member, peer):
            ref = block(member)
            return remote(ref, ref, side_send.at[slot + distance], side_recv.at[slot + distance], {"tp": peer})

        def out():
            for distance, member in enumerate(line):
                copy(distance, t, member).start()

        def arrive():
            for distance in range(ring - 1):
                source = lax.rem(t + ring - 1 - distance, ring)
                copy(distance, source, source).wait_recv()

        def finish():
            for distance, member in enumerate(line):
                copy(distance, t, member).wait_send()

        return out, arrive, finish

    for step in range(STEPS):
        text_load(step).start()
    up_load = pltpu.make_async_copy(merger_up, up_held, load_sem.at[0])
    for step in range(4):
        line_own(step)
    for step in range(STEPS):
        for load in weight_loads(step):
            load.start()

    def open_weights(step, carry):
        for load in weight_loads(step):
            load.wait()
        send(X_OWN, step)
        send(CORE_OWN, step)
        return carry

    lax.fori_loop(0, STEPS, open_weights, 0)

    def attend(qkv_held, proj_held):
        loads = [
            pltpu.make_async_copy(vit_qkv, qkv_held, load_sem.at[1]),
            pltpu.make_async_copy(vit_proj, proj_held, load_sem.at[2]),
        ]
        for load in loads:
            load.start()
        up_load.start()
        normed = layer_norm(patches[...].astype(jnp.float32), vit_gain[...].reshape(1, -1)).astype(jnp.bfloat16)
        loads[0].wait()
        queries, keys, values = [
            lax.dot_general(
                normed, qkv_held[entry], (((1,), (1,)), ((), ())), preferred_element_type=jnp.float32
            )
            for entry in range(3)
        ]
        keys = keys.astype(jnp.bfloat16)
        count = patches.shape[0]
        row = lax.broadcasted_iota(jnp.int32, (count, count), 0) // MAXP
        column = lax.broadcasted_iota(jnp.int32, (count, count), 1) // MAXP
        index = lax.broadcasted_iota(jnp.int32, (1, count), 1)
        limit = jnp.zeros((1, count), jnp.int32)
        for image in range(IMG_DEV):
            limit = jnp.where(index // MAXP == image, image * MAXP + patch_counts[w * IMG_DEV + image], limit)
        seen = (row == column) & (index < limit)
        lane = lax.broadcasted_iota(jnp.int32, queries.shape, 1) // VHD
        context = jnp.zeros(queries.shape, jnp.float32)
        for head in range(queries.shape[1] // VHD):
            own = lane == head
            scores = lax.dot_general(
                jnp.where(own, queries, 0.0).astype(jnp.bfloat16),
                keys,
                (((1,), (1,)), ((), ())),
                preferred_element_type=jnp.float32,
            ) * VHD ** (-0.5)
            scores = jnp.where(seen, scores, -jnp.inf)
            raised = jnp.exp(scores - jnp.max(scores, axis=-1, keepdims=True))
            probs = (raised / jnp.sum(raised, axis=-1, keepdims=True)).astype(jnp.bfloat16)
            context = context + jnp.dot(
                probs, jnp.where(own, values, 0.0).astype(jnp.bfloat16), preferred_element_type=jnp.float32
            )
        loads[1].wait()
        part[...] = jnp.dot(
            context.astype(jnp.bfloat16), proj_held[...], preferred_element_type=jnp.float32
        ).astype(jnp.bfloat16)

    pl.run_scoped(attend, pltpu.VMEM(vit_qkv.shape, jnp.bfloat16), pltpu.VMEM(vit_proj.shape, jnp.bfloat16))

    own_rows = part.shape[0] // ring

    def share_piece(member):
        return part.at[pl.ds(pl.multiple_of(member * own_rows, own_rows), own_rows)]

    hand_in, swap, hand_back, result, finish_shares = scatter(
        0, share_piece, shares_relay, shares_crossed, shares_sum, shares_in
    )
    hand_in()
    line_own(4)
    line_pass(1, 0)
    swap()
    line_pass(1, 1)
    line_pass(2, 0)
    hand_back()
    line_own(5)
    line_pass(1, 2)
    for step in range(3):
        pass_on(step)
    total[...] = jnp.zeros_like(total)
    squares[...] = jnp.zeros_like(squares)
    handoff_masks(w, wide, visuals.shape[2], patch_counts, placement, pick, place)
    taken = jnp.sum(place[...].astype(jnp.float32), axis=1, keepdims=True)
    keep[...] = jnp.broadcast_to(1.0 - taken, keep.shape)
    rotary_tables(positions, inverse, cosine, sine)

    own_patches = patches[pl.ds(pl.multiple_of(t * own_rows, own_rows), own_rows)]
    mixed = own_patches.astype(jnp.float32) + result()
    normed = layer_norm(mixed, merger_gain[...].reshape(1, -1)).astype(jnp.bfloat16)
    joined = merged.shape[0]
    chosen = (own_rows // joined, own_rows)
    row, column = lax.broadcasted_iota(jnp.int32, chosen, 0), lax.broadcasted_iota(jnp.int32, chosen, 1)
    for entry in range(joined):
        picks = (column == row * joined + entry).astype(jnp.float32).astype(jnp.bfloat16)
        merged[entry, t] = jnp.dot(picks, normed, preferred_element_type=jnp.float32).astype(jnp.bfloat16)
    out, arrive, finish_merged = gather(6, lambda member: merged.at[:, member])
    out()
    line_pass(2, 1)
    line_own(6)
    line_pass(1, 3)
    for step in range(3, 5):
        pass_on(step)
    for step in range(2):
        pass_core(step)
    arrive()

    up_load.wait()
    rows = own_rows // joined * ring
    inner = merged.shape[-1]
    raised = None
    for entry in range(joined):
        term = jnp.dot(
            merged[entry].reshape(rows, inner),
            up_held[pl.ds(entry * inner, inner)],
            preferred_element_type=jnp.float32,
        )
        raised = term if raised is None else raised + term
    hidden[...] = (0.5 * raised * (1.0 + lax.erf(raised * 0.5**0.5))).astype(jnp.bfloat16)

    features = visuals.shape[-1]
    tile = features // 4
    hand_in, swap, hand_back, result, finish_visual = scatter(
        9, lambda member: visual_part.at[member], visual_relay, visual_crossed, visual_sum, visual_in
    )

    def project_down(down_held):
        def load(member, slot):
            columns = pl.ds(pl.multiple_of(member * features, features), features)
            return pltpu.make_async_copy(merger_down.at[:, columns], down_held.at[slot], load_sem.at[3 + slot])

        def make(member, slot):
            load(member, slot).wait()

            def column(entry, carry):
                columns = pl.ds(pl.multiple_of(entry * tile, tile), tile)
                visual_part[member, :, columns] = jnp.dot(
                    hidden[...], down_held[slot, :, columns], preferred_element_type=jnp.float32
                ).astype(jnp.bfloat16)
                return carry

            lax.fori_loop(0, features // tile, column, 0)

        order = (half_start, half_start + 1, near, t)
        load(order[0], 0).start()
        load(order[1], 1).start()
        make(order[0], 0)
        load(order[2], 0).start()
        make(order[1], 1)
        load(order[3], 1).start()
        make(order[2], 0)
        hand_in()
        make(order[3], 1)

    pl.run_scoped(project_down, pltpu.VMEM((2, merger_down.shape[0], features), jnp.bfloat16))
    line_pass(2, 2)
    line_own(7)
    line_pass(1, 4)
    for step in range(5, 7):
        pass_on(step)
    for step in range(2, 4):
        pass_core(step)
    swap()
    line_pass(2, 3)
    hand_back()
    line_pass(1, 5)
    for step in range(7, STEPS):
        pass_on(step)

    picked = result().astype(jnp.bfloat16)
    packed[...] = (
        jnp.dot(pick[...], picked, preferred_element_type=jnp.float32)
        .astype(jnp.bfloat16)
        .reshape(packed.shape)
    )
    visuals[t, w] = packed[w]
    hand = [
        remote(packed.at[owner], visuals.at[t, w], side_send.at[15 + entry], side_recv.at[15 + entry], {"wide": owner})
        for entry, owner in enumerate((core, across, diagonal))
    ]
    for copy in hand:
        copy.start()
    line_pass(2, 4)
    for step in range(4, 6):
        pass_core(step)
    for entry, owner in enumerate((core, across, diagonal)):
        block = visuals.at[t, owner]
        remote(block, block, side_send.at[15 + entry], side_recv.at[15 + entry], {"wide": owner}).wait_recv()
    out, arrive, finish_rows = gather(18, lambda member: visuals.at[member])
    out()
    line_pass(1, 6)
    for step in range(6, STEPS):
        pass_core(step)
    line_pass(2, 5)
    arrive()
    line_pass(1, 7)

    width = total.shape[1] // 3
    slots = place.shape[1]

    def consume(step, carry):
        @pl.when(step < STEPS - 6)
        def _():
            line_pass(2, step + 6)

        for kind in (CORE_OWN, CORE_X, CORE_Y):
            received(kind, step)
        line_received(ring - 2, step)
        columns = pl.ds(pl.multiple_of(step * depth, depth), depth)
        for block in range(ring):
            brought = jnp.dot(
                place[...],
                visuals[block, :, :, columns].reshape(slots, depth),
                preferred_element_type=jnp.float32,
            )
            values = texts[block, step].astype(jnp.float32) * keep[...] + brought
            folded = values * values
            lanes = squares.shape[1]
            for start in range(0, depth, lanes):
                squares[...] += folded[:, start : start + lanes]
            scale = gain[pl.ds(pl.multiple_of(block * features + step * depth, depth), depth)].reshape(1, -1)
            scaled[:, block * depth : (block + 1) * depth] = (values * scale).astype(jnp.bfloat16)

        def column(entry, carry):
            across_columns = pl.ds(pl.multiple_of(entry * width, width), width)
            added = total[:, across_columns]
            for block in range(wide):
                added = added + jnp.dot(
                    scaled[:, block * depth : (block + 1) * depth],
                    weights[block, pl.ds(pl.multiple_of(step * depth, depth), depth), across_columns],
                    preferred_element_type=jnp.float32,
                )
            total[:, across_columns] = added
            return carry

        return lax.fori_loop(0, 3, column, carry)

    lax.fori_loop(0, STEPS, consume, 0)

    square = jnp.sum(squares[...], axis=1, keepdims=True) / gain.shape[0]
    squares[...] = jnp.broadcast_to(lax.rsqrt(square + NORM_EPS), squares.shape)

    def turned(start):
        values = total[:, pl.ds(start, HD)] * squares[...]
        return (values * cosine[...] + pltpu.roll(values, HD // 2, 1) * sine[...]).astype(jnp.bfloat16)

    def turned_head(entry, carry):
        start = pl.multiple_of(entry * HD, HD)
        rows_out[:, pl.ds(start, HD)] = turned(start)
        return carry

    lax.fori_loop(0, second // HD, turned_head, 0)
    for start in range(second, total.shape[1], HD):
        values = total[:, start : start + HD] * squares[...]
        rows_out[:, start : start + HD] = values.astype(jnp.bfloat16)

    def drain(step, carry):
        for kind in range(LINE):
            sent(kind, step)
        for hop in range(ring - 1):
            line_send(hop, step, lambda copy: copy.wait_send())
        return carry

    lax.fori_loop(0, STEPS, drain, 0)
    finish_shares()
    finish_merged()
    finish_visual()
    finish_rows()
    for copy in hand:
        copy.wait_send()


def split_columns(rows, *results):
    start = 0
    for result in results:
        result[...] = rows[:, start : start + result.shape[1]]
        start += result.shape[1]


def handoff_masks(owner, wide, capacity, patch_counts, placement, pick, place):
    def grid(ref):
        return [lax.broadcasted_iota(jnp.int32, ref.shape, axis) for axis in range(2)]

    slot, row = grid(pick)
    token, place_slot = grid(place)
    picked, placed = jnp.zeros(pick.shape, jnp.float32), jnp.zeros(place.shape, jnp.float32)
    for source in range(wide):
        images = [source * IMG_DEV + entry for entry in range(IMG_DEV)]
        owners = [placement[0, image] for image in images]
        counts = [patch_counts[image] // 4 for image in images]
        mine = jnp.where(owner == source, 1, 0)
        for entry, image in enumerate(images):
            offset = 0
            for earlier in range(entry):
                offset = offset + jnp.where(owners[earlier] == owners[entry], counts[earlier], 0)
            start = owners[entry] * capacity + offset
            live = (slot >= start) & (slot < start + counts[entry] * mine)
            picked = jnp.where(live & (row - slot == entry * MAXM - start), 1.0, picked)
            begin = placement[1, image]
            length = jnp.where(owners[entry] == owner, counts[entry], 0)
            inside = (token >= begin) & (token < begin + length)
            placed = jnp.where(inside & (place_slot - token == source * capacity + offset - begin), 1.0, placed)
    pick[...] = picked.astype(pick.dtype)
    place[...] = placed.astype(place.dtype)


def rotary_tables(positions, inverse, cosine, sine):
    lane = lax.broadcasted_iota(jnp.int32, cosine.shape, 1)
    ordinal = lax.rem(lane, HD // 2)
    wanted = positions[...].astype(jnp.float32)
    wanted = jnp.concatenate([wanted, jnp.zeros((8 - wanted.shape[0], wanted.shape[1]), jnp.float32)], axis=0).T
    first_end = HD // 8
    second = first_end + 3 * HD // 16
    chosen = jnp.where(
        ordinal < first_end, wanted[:, 0:1], jnp.where(ordinal < second, wanted[:, 1:2], wanted[:, 2:3])
    )
    angles = chosen * inverse[...]
    cosine[...] = jnp.cos(angles)
    turned = jnp.sin(angles)
    sine[...] = jnp.where(lane < HD // 2, -turned, turned)


def per_device_kernel(
    patches,
    patch_counts,
    placement,
    positions,
    text_embeds,
    vit_gain,
    vit_qkv,
    vit_proj,
    merger_gain,
    merger_up,
    merger_down,
    llm_gain,
    llm_query,
    llm_key,
    llm_value,
):
    wide, ring = lax.axis_size("wide"), lax.axis_size("tp")
    capacity = MAXM * ((IMG_DEV + wide - 1) // wide)
    merged_rows = IMG_DEV * MAXM
    slots = wide * capacity
    frequency = jnp.arange(HD).astype(jnp.float32) % (HD // 2)
    inverse = (ROPE_BASE ** (-2.0 * frequency / HD)).reshape(1, HD)
    tokens, features = text_embeds.shape
    depth_all = llm_query.shape[0]
    columns = llm_query.shape[1] + llm_key.shape[1] + llm_value.shape[1]
    depth = depth_all // STEPS
    own_rows = patches.shape[0] // ring
    joined = merger_up.shape[0] // VD
    hidden_units = merger_up.shape[1]
    bf16, f32 = jnp.bfloat16, jnp.float32
    smem, vmem = pl.BlockSpec(memory_space=pltpu.SMEM), pl.BlockSpec(memory_space=pltpu.VMEM)
    anywhere = pl.BlockSpec(memory_space=pl.ANY)
    rows = pl.pallas_call(
        prompt_kernel,
        out_shape=jax.ShapeDtypeStruct((tokens, columns), bf16),
        in_specs=[smem] * 2 + [vmem] * 4 + [anywhere] * 2 + [vmem] + [anywhere] * 3 + [vmem] + [anywhere] * 3,
        out_specs=vmem,
        scratch_shapes=[
            pltpu.VMEM((wide, depth_all, columns), bf16),
            pltpu.VMEM((ring, STEPS, tokens, depth), bf16),
            pltpu.VMEM((tokens, columns), f32),
            pltpu.VMEM((tokens, HD), f32),
            pltpu.VMEM((tokens, depth), f32),
            pltpu.VMEM((tokens, ring * depth), bf16),
            pltpu.VMEM(merger_up.shape, bf16),
            pltpu.VMEM(patches.shape, bf16),
            pltpu.VMEM((2, own_rows, VD), bf16),
            pltpu.VMEM((2, own_rows, VD), bf16),
            pltpu.VMEM((3, own_rows, VD), bf16),
            pltpu.VMEM((own_rows, VD), bf16),
            pltpu.VMEM((joined, ring, own_rows // joined, VD), bf16),
            pltpu.VMEM((merged_rows, hidden_units), bf16),
            pltpu.VMEM((ring, merged_rows, features), bf16),
            pltpu.VMEM((2, merged_rows, features), bf16),
            pltpu.VMEM((2, merged_rows, features), bf16),
            pltpu.VMEM((3, merged_rows, features), bf16),
            pltpu.VMEM((merged_rows, features), bf16),
            pltpu.VMEM((wide, capacity, features), bf16),
            pltpu.VMEM((ring, wide, capacity, features), bf16),
            pltpu.VMEM((slots, merged_rows), bf16),
            pltpu.VMEM((tokens, slots), bf16),
            pltpu.VMEM((tokens, HD), f32),
            pltpu.VMEM((tokens, HD), f32),
            pltpu.SemaphoreType.DMA((4, STEPS)),
            pltpu.SemaphoreType.DMA((5,)),
            pltpu.SemaphoreType.DMA((LINE + 2 * (ring - 1), STEPS)),
            pltpu.SemaphoreType.DMA((LINE + 2 * (ring - 1), STEPS)),
            pltpu.SemaphoreType.DMA((18 + ring - 1,)),
            pltpu.SemaphoreType.DMA((18 + ring - 1,)),
        ],
        compiler_params=pltpu.CompilerParams(
            collective_id=0, has_side_effects=True, vmem_limit_bytes=67043328
        ),
    )(
        patch_counts,
        placement.T,
        inverse,
        positions,
        patches,
        vit_gain,
        jnp.transpose(vit_qkv, (1, 2, 0)),
        vit_proj,
        merger_gain,
        merger_up,
        merger_down,
        text_embeds,
        llm_gain,
        llm_query,
        llm_key,
        llm_value,
    )

    share = tokens // 4
    return pl.pallas_call(
        split_columns,
        grid=(4,),
        out_shape=[
            jax.ShapeDtypeStruct((tokens, weight.shape[1]), bf16)
            for weight in (llm_query, llm_key, llm_value)
        ],
        in_specs=[pl.BlockSpec((share, columns), lambda step: (step, 0))],
        out_specs=[
            pl.BlockSpec((share, weight.shape[1]), lambda step: (step, 0))
            for weight in (llm_query, llm_key, llm_value)
        ],
    )(rows)


def solution(mesh):
    ring = mesh.shape["tp"] == 4 and mesh.shape["wide"] == 4 and mesh.shape["groups"] == 2
    return jax.shard_map(
        per_device_kernel if ring else per_device_rings,
        mesh=mesh,
        in_specs=(
            P(("groups", "wide"), None),
            P("groups"),
            P("groups", None),
            P(None, ("groups", "wide")),
            P(("groups", "wide"), "tp"),
            P(),
            P(None, None, "tp"),
            P("tp", None),
            P(),
            P(None, "tp"),
            P("tp", None),
            P(),
            P("wide", "tp"),
            P("wide", "tp"),
            P("wide", "tp"),
        ),
        out_specs=(
            P(("groups", "wide"), "tp"),
            P(("groups", "wide"), "tp"),
            P(("groups", "wide"), "tp"),
        ),
        check_vma=False,
    )
```

```python
import jax
import jax.numpy as jnp
from jax import lax
from jax.experimental import pallas as pl
from jax.experimental.pallas import tpu as pltpu
from jax.sharding import PartitionSpec as P

VD = 1280
HD = 128
IMG_DEV = 8
MAXP = 32
TOK_DEV = 512
VHD = 80
MAXM = 8


NORM_EPS = 1e-06
ROPE_BASE = 1000000.0


def layer_norm(inputs, scale_gain):
    center = jnp.mean(inputs, axis=-1, keepdims=True)
    shifted = inputs - center
    spread = jnp.mean(shifted * shifted, axis=-1, keepdims=True)
    return shifted * lax.rsqrt(spread + NORM_EPS) * scale_gain


def rms_norm(inputs, scale_gain):
    square = jnp.mean(inputs * inputs, axis=-1, keepdims=True)
    return inputs * lax.rsqrt(square + NORM_EPS) * scale_gain


def rotary(values, positions):
    half_size = HD // 2
    frequency = jnp.arange(half_size).astype(jnp.float32)
    inverse = ROPE_BASE ** (-2.0 * frequency / HD)
    first_end = HD // 8
    second = first_end + 3 * HD // 16
    ordinal = jnp.arange(half_size)
    section = jnp.where(ordinal < first_end, 0, jnp.where(ordinal < second, 1, 2))
    chosen = jnp.where(
        section[:, None] == 0,
        positions[0][None, :],
        jnp.where(section[:, None] == 1, positions[1][None, :], positions[2][None, :]),
    )
    angles = chosen.T.astype(jnp.float32) * inverse[None, :]
    angles = jnp.concatenate([angles, angles], axis=1)
    cosine = jnp.cos(angles)[:, None, :]
    sine_table = jnp.sin(angles)[:, None, :]
    upper_half = values[..., :half_size]
    lower_half = values[..., half_size:]
    turned = jnp.concatenate([-lower_half, upper_half], axis=-1)
    return values * cosine + turned * sine_table


def handoff_tables(patch_counts, placement, width_wide, myself, capacity):
    merged_count = patch_counts // 4
    owners = placement[:, 0]
    starts = placement[:, 1]
    owner_grid = owners.reshape(width_wide, IMG_DEV)
    count_grid = merged_count.reshape(width_wide, IMG_DEV)
    ordinal = jnp.arange(IMG_DEV)
    before = ordinal[:, None] < ordinal[None, :]
    same_owner = owner_grid[:, :, None] == owner_grid[:, None, :]
    offsets = jnp.sum(jnp.where(same_owner & before[None], count_grid[:, :, None], 0), axis=1)
    mine_owner = lax.dynamic_index_in_dim(owner_grid, myself, 0, keepdims=False)
    mine_count = lax.dynamic_index_in_dim(count_grid, myself, 0, keepdims=False)
    mine_offset = lax.dynamic_index_in_dim(offsets, myself, 0, keepdims=False)
    target = jnp.arange(width_wide)[:, None, None]
    slot_index = jnp.arange(capacity)[None, :, None]
    matches = (
        (mine_owner[None, None, :] == target)
        & (slot_index >= mine_offset[None, None, :])
        & (slot_index < mine_offset[None, None, :] + mine_count[None, None, :])
    )
    source_row = ordinal[None, None, :] * MAXM + slot_index - mine_offset[None, None, :]
    send_index = jnp.sum(jnp.where(matches, source_row, 0), axis=-1)
    send_live = jnp.any(matches, axis=-1)
    row_place = jnp.arange(TOK_DEV)[:, None]
    inside = (
        (owners[None, :] == myself)
        & (row_place >= starts[None, :])
        & (row_place < starts[None, :] + merged_count[None, :])
    )
    image_source = jnp.arange(owners.shape[0]) // IMG_DEV
    flat_slot = (
        image_source[None, :] * capacity
        + offsets.reshape(-1)[None, :]
        + row_place
        - starts[None, :]
    )
    take_index = jnp.sum(jnp.where(inside, flat_slot, 0), axis=-1)
    take_live = jnp.any(inside, axis=-1)
    return (send_index, send_live, take_index, take_live)


def pack_rows(visual, send_index, send_live):
    picked = jnp.take(visual, send_index.reshape(-1), axis=0)
    picked = picked.reshape(send_index.shape + (visual.shape[1],))
    return jnp.where(send_live[..., None], picked, jnp.zeros((), visual.dtype))


def exchange_sum(partial, axis_name, split_axis):
    members = lax.axis_size(axis_name)
    shape = partial.shape
    cut = shape[:split_axis] + (members, shape[split_axis] // members) + shape[split_axis + 1 :]
    stacked = jnp.moveaxis(partial.reshape(cut), split_axis, 0)
    swapped = lax.all_to_all(stacked, axis_name, split_axis=0, concat_axis=0, tiled=True)
    return jnp.sum(swapped.astype(jnp.float32), axis=0)


def doubling_gather(block, axis_name):
    members = lax.axis_size(axis_name)
    held = {0: block}
    bits = []
    step = 1
    while step < members:
        bits.append(step)
        step *= 2
    for bit in bits[1:] + bits[:1]:
        pairs = [(source, source ^ bit) for source in range(members)]
        for entry in sorted(held):
            held[entry ^ bit] = lax.ppermute(held[entry], axis_name, pairs)
    return [held[entry] for entry in range(members)]


def ring_gather_columns(block, axis_name):
    members = lax.axis_size(axis_name)
    me = lax.axis_index(axis_name)
    width = block.shape[1]
    up = [(source, (source + 1) % members) for source in range(members)]
    down = [(source, (source - 1) % members) for source in range(members)]
    gathered = jnp.zeros((block.shape[0], width * members), block.dtype)
    pieces = [(0, 0, block)]
    forward, backward = block, block
    distance = 1
    while 2 * distance < members:
        forward = lax.ppermute(forward, axis_name, up)
        backward = lax.ppermute(backward, axis_name, down)
        pieces.append((members - distance, 0, forward))
        pieces.append((distance, 0, backward))
        distance += 1
    if 2 * distance == members:
        half = width // 2
        pieces.append((distance, 0, lax.ppermute(forward[:, :half], axis_name, up)))
        pieces.append((distance, half, lax.ppermute(backward[:, half:], axis_name, down)))
    for offset, inner, piece in pieces:
        column = lax.rem(me + offset, members) * width + inner
        gathered = lax.dynamic_update_slice(gathered, piece, (0, column))
    return gathered


def project(rows, weight_blocks, member):
    depth = weight_blocks[0].shape[0]
    total = None
    for entry, block in enumerate(weight_blocks):
        columns = lax.dynamic_slice_in_dim(rows, (member ^ entry) * depth, depth, 1)
        share = jnp.dot(columns, block, preferred_element_type=jnp.float32)
        total = share if total is None else total + share
    return total


def per_device_rings(
    patches,
    patch_counts,
    placement,
    positions,
    text_embeds,
    vit_gain,
    vit_qkv,
    vit_proj,
    merger_gain,
    merger_up,
    merger_down,
    llm_gain,
    llm_query,
    llm_key,
    llm_value,
):
    width_wide = lax.axis_size("wide")
    myself = lax.axis_index("wide")
    capacity = MAXM * ((IMG_DEV + width_wide - 1) // width_wide)
    local_heads = vit_qkv.shape[2] // VHD
    own_weights = jnp.concatenate([llm_query, llm_key, llm_value], axis=1)
    weight_blocks = doubling_gather(own_weights, "wide")
    text_rows = ring_gather_columns(text_embeds, "tp")
    members = lax.axis_size("tp")
    patch_rows = patches.astype(jnp.float32)
    normed = layer_norm(patch_rows, vit_gain).astype(jnp.bfloat16)
    triple = jnp.dot(normed, vit_qkv.reshape(VD, -1), preferred_element_type=jnp.float32).astype(
        jnp.bfloat16
    )
    triple = triple.reshape(IMG_DEV, MAXP, 3, local_heads, VHD)
    scores = jnp.einsum(
        "iqhd,ikhd->ihqk", triple[:, :, 0], triple[:, :, 1], preferred_element_type=jnp.float32
    ) * VHD ** (-0.5)
    own_counts = lax.dynamic_slice_in_dim(patch_counts, myself * IMG_DEV, IMG_DEV)
    present = jnp.arange(MAXP)[None, :] < own_counts[:, None]
    scores = jnp.where(present[:, None, None, :], scores, -jnp.inf)
    highest = jnp.max(scores, axis=-1, keepdims=True)
    raised = jnp.exp(scores - highest)
    attention_weights = (raised / jnp.sum(raised, axis=-1, keepdims=True)).astype(jnp.bfloat16)
    context = jnp.einsum(
        "ihqk,ikhd->iqhd", attention_weights, triple[:, :, 2], preferred_element_type=jnp.float32
    ).astype(jnp.bfloat16)
    context = context.reshape(IMG_DEV * MAXP, local_heads * VHD)
    partial_heads = jnp.dot(context, vit_proj, preferred_element_type=jnp.float32)
    attended = exchange_sum(partial_heads.astype(jnp.bfloat16), "tp", 0)
    own_rows = IMG_DEV * MAXP // members
    own_patches = lax.dynamic_slice_in_dim(patches, lax.axis_index("tp") * own_rows, own_rows, 0)
    mixed_rows = own_patches.astype(jnp.float32) + attended
    own_merged = layer_norm(mixed_rows, merger_gain).astype(jnp.bfloat16)
    own_merged = own_merged.reshape(own_rows * MAXM // MAXP, 4 * VD)
    merged_in = lax.all_gather(own_merged, "tp", axis=0, tiled=True)
    hidden = jax.nn.gelu(
        jnp.dot(merged_in, merger_up, preferred_element_type=jnp.float32), approximate=False
    ).astype(jnp.bfloat16)
    partial_visual = jnp.dot(hidden, merger_down, preferred_element_type=jnp.float32)
    send_index, send_live, take_index, take_live = handoff_tables(
        patch_counts, placement, width_wide, myself, capacity
    )
    visual = exchange_sum(partial_visual.astype(jnp.bfloat16), "tp", 1).astype(jnp.bfloat16)
    outgoing = pack_rows(visual, send_index, send_live)
    incoming = lax.all_to_all(outgoing, "wide", split_axis=0, concat_axis=0, tiled=True)
    incoming = incoming.reshape(-1, incoming.shape[-1])
    copies = jnp.broadcast_to(incoming[None], (members,) + incoming.shape)
    spread_rows = lax.all_to_all(copies, "tp", split_axis=0, concat_axis=0, tiled=True)
    visual_rows = jnp.swapaxes(spread_rows, 0, 1).reshape(incoming.shape[0], -1)
    normed_text = rms_norm(text_rows.astype(jnp.float32), llm_gain).astype(jnp.bfloat16)
    normed_visual = rms_norm(visual_rows.astype(jnp.float32), llm_gain).astype(jnp.bfloat16)
    projected_text = project(normed_text, weight_blocks, myself)
    projected_visual = project(normed_visual, weight_blocks, myself)
    placed = jnp.take(projected_visual, take_index, axis=0)
    projected = jnp.where(take_live[:, None], placed, projected_text)
    first = llm_query.shape[1]
    second = first + llm_key.shape[1]
    projected_query = projected[:, :first]
    projected_key = projected[:, first:second]
    projected_value = projected[:, second:]
    queries = (
        rotary(projected_query.reshape(TOK_DEV, -1, HD), positions)
        .astype(jnp.bfloat16)
        .reshape(TOK_DEV, -1)
    )
    key_rows = (
        rotary(projected_key.reshape(TOK_DEV, -1, HD), positions)
        .astype(jnp.bfloat16)
        .reshape(TOK_DEV, -1)
    )
    value_rows = projected_value.astype(jnp.bfloat16)
    return (queries, key_rows, value_rows)


STEPS = 8
LEAST_MERGED = 6
MESH = pl.DeviceIdType.MESH
X_OWN, Y_PASS, CORE_OWN, CORE_X, CORE_Y, LINE = range(6)


def prompt_kernel(
    patch_counts,
    placement,
    inverse,
    positions,
    patches,
    vit_gain,
    vit_qkv,
    vit_proj,
    merger_gain,
    merger_up,
    merger_down,
    text,
    gain,
    w_query,
    w_key,
    w_value,
    rows_out,
    expand,
    place,
    weights,
    texts,
    total,
    squares,
    scaled,
    compact,
    up_held,
    part,
    shares_relay,
    shares_crossed,
    shares_sum,
    shares_in,
    merged,
    hidden,
    visual_part,
    visual_relay,
    visual_crossed,
    visual_sum,
    visual_in,
    packed,
    visuals,
    pick,
    place_rows,
    cosine,
    sine,
    local_sem,
    load_sem,
    bulk_send,
    bulk_recv,
    side_send,
    side_recv,
):
    groups, wide, ring = lax.axis_size("groups"), lax.axis_size("wide"), lax.axis_size("tp")
    g, w, t = lax.axis_index("groups"), lax.axis_index("wide"), lax.axis_index("tp")
    core = w + 1 - 2 * lax.rem(w, 2)
    across = lax.rem(w + 2, wide)
    diagonal = across + 1 - 2 * lax.rem(across, 2)
    other = lax.rem(g + 1, groups)
    above, below = {"tp": lax.rem(t + 1, ring)}, {"tp": lax.rem(t + ring - 1, ring)}
    depth = weights.shape[1] // wide
    half = depth // groups
    first, second = w_query.shape[1], w_query.shape[1] + w_key.shape[1]
    line = [lax.rem(t + distance, ring) for distance in range(1, ring)]

    barrier = pltpu.get_barrier_semaphore()
    peers = [{"tp": member} for member in line]
    peers += [{"wide": core}, {"wide": across}, {"wide": diagonal}, {"groups": other}]
    for peer in peers:
        pl.semaphore_signal(barrier, inc=1, device_id=peer, device_id_type=MESH)
    pl.semaphore_wait(barrier, len(peers))

    def remote(source, target, send, recv, peer):
        return pltpu.make_async_remote_copy(
            src_ref=source,
            dst_ref=target,
            send_sem=send,
            recv_sem=recv,
            device_id=peer,
            device_id_type=MESH,
        )

    def in_place(kind, step, ref, peer):
        return remote(ref, ref, bulk_send.at[kind, step], bulk_recv.at[kind, step], peer)

    def rows_of(block, step, offset, count):
        start = pl.multiple_of(block * depth + offset, 16)
        return weights.at[step, pl.ds(start, count)]

    bulk = {
        X_OWN: (lambda s: rows_of(w, s, g * half, half), lambda s: rows_of(across, s, g * half, half), {"wide": across}),
        Y_PASS: (lambda s: rows_of(across, s, g * half, half), lambda s: rows_of(across, s, other * half, half), {"groups": other}),
        CORE_OWN: (lambda s: rows_of(w, s, 0, depth), lambda s: rows_of(core, s, 0, depth), {"wide": core}),
        CORE_X: (lambda s: rows_of(across, s, g * half, half), lambda s: rows_of(diagonal, s, g * half, half), {"wide": core}),
        CORE_Y: (lambda s: rows_of(across, s, other * half, half), lambda s: rows_of(diagonal, s, other * half, half), {"wide": core}),
    }

    def send(kind, step):
        in_place(kind, step, bulk[kind][0](step), bulk[kind][2]).start()

    def sent(kind, step):
        in_place(kind, step, bulk[kind][0](step), bulk[kind][2]).wait_send()

    def received(kind, step):
        in_place(kind, step, bulk[kind][1](step), bulk[kind][2]).wait_recv()

    def weight_loads(step):
        rows = pl.ds(pl.multiple_of(step * depth, depth), depth)
        return [
            pltpu.make_async_copy(
                ref.at[rows], rows_of(w, step, 0, depth).at[:, pl.ds(start, ref.shape[1])], local_sem.at[entry, step]
            )
            for entry, (ref, start) in enumerate(((w_query, 0), (w_key, first), (w_value, second)))
        ]

    def text_load(raw, step):
        columns = pl.ds(pl.multiple_of(step * depth, depth), depth)
        return pltpu.make_async_copy(text.at[:, columns], raw.at[step], local_sem.at[3, step])

    def up_copy(hop, step, block):
        return in_place(LINE + hop, step, texts.at[block, step], above)

    def down_copy(hop, step, block):
        return in_place(LINE + ring - 1 + hop, step, texts.at[block, step], below)

    def line_send(hop, step, act=lambda copy: copy.start()):
        @pl.when(t + 1 < ring)
        def _():
            @pl.when(t >= hop)
            def _():
                act(up_copy(hop, step, t - hop))

        @pl.when(t > 0)
        def _():
            @pl.when(t + hop < ring)
            def _():
                act(down_copy(hop, step, t + hop))

    def line_received(hop, step):
        @pl.when(t > hop)
        def _():
            up_copy(hop, step, t - 1 - hop).wait_recv()

        @pl.when(t + 1 + hop < ring)
        def _():
            down_copy(hop, step, t + 1 + hop).wait_recv()

    def line_own(step):
        line_send(0, step)

    def line_pass(hop, step):
        line_received(hop - 1, step)
        line_send(hop, step)

    def pass_on(step):
        received(X_OWN, step)
        send(Y_PASS, step)
        send(CORE_X, step)

    def pass_core(step):
        received(Y_PASS, step)
        send(CORE_Y, step)

    near = t + 1 - 2 * lax.rem(t, 2)
    beyond = ring - 1 - t
    half_start = ring // 2 * lax.rem(t // 2 + 1, 2)
    inner_member = lax.rem(t // 2 + t, 2) == 1
    outer_member = jnp.logical_not(inner_member)

    def scatter(slot, pieces, relay, crossed, summed, arrived):
        def copy(entry, source, target, member):
            return remote(source, target, side_send.at[slot + entry], side_recv.at[slot + entry], {"tp": member})

        def hand_in(act=lambda copied: copied.start()):
            @pl.when(outer_member)
            def _():
                for entry in range(2):
                    act(copy(entry, pieces(half_start + entry), relay.at[entry], near))
                act(copy(2, pieces(near), arrived, near))

        def swap():
            @pl.when(outer_member)
            def _():
                crossed[...] = jnp.zeros_like(crossed)

            @pl.when(inner_member)
            def _():
                for entry in range(2):
                    copy(entry, relay.at[entry], relay.at[entry], near).wait_recv()
                    added = relay[entry].astype(jnp.float32) + pieces(half_start + entry)[...].astype(jnp.float32)
                    summed[entry] = added.astype(summed.dtype)
                for entry in range(2):
                    copy(3 + entry, summed.at[entry], crossed.at[entry], beyond).start()

        def hand_back():
            @pl.when(inner_member)
            def _():
                for entry in range(2):
                    copy(3 + entry, crossed.at[entry], crossed.at[entry], beyond).wait_recv()
                added = crossed[lax.rem(near, 2)].astype(jnp.float32) + pieces(near)[...].astype(jnp.float32)
                summed[2] = added.astype(summed.dtype)
                copy(5, summed.at[2], arrived, near).start()

        def result():
            @pl.when(inner_member)
            def _():
                copy(2, arrived, arrived, near).wait_recv()

            @pl.when(outer_member)
            def _():
                copy(5, arrived, arrived, near).wait_recv()

            own = pieces(t)[...].astype(jnp.float32)
            return own + arrived[...].astype(jnp.float32) + crossed[lax.rem(t, 2)].astype(jnp.float32)

        def finish():
            hand_in(lambda copied: copied.wait_send())

            @pl.when(inner_member)
            def _():
                for entry in range(2):
                    copy(3 + entry, summed.at[entry], crossed.at[entry], beyond).wait_send()
                copy(5, summed.at[2], arrived, near).wait_send()

        return hand_in, swap, hand_back, result, finish

    def gather(slot, block):
        def copy(distance, member, peer):
            ref = block(member)
            return remote(ref, ref, side_send.at[slot + distance], side_recv.at[slot + distance], {"tp": peer})

        def out():
            for distance, member in enumerate(line):
                copy(distance, t, member).start()

        def arrive():
            for distance in range(ring - 1):
                source = lax.rem(t + ring - 1 - distance, ring)
                copy(distance, source, source).wait_recv()

        def finish():
            for distance, member in enumerate(line):
                copy(distance, t, member).wait_send()

        return out, arrive, finish

    up_load = pltpu.make_async_copy(merger_up, up_held, load_sem.at[0])
    for step in range(STEPS):
        for load in weight_loads(step):
            load.start()

    def compact_text(raw):
        for step in range(STEPS):
            text_load(raw, step).start()
        token = lax.broadcasted_iota(jnp.int32, (1, compact.shape[1]), 1)
        slot = lax.broadcasted_iota(jnp.int32, compact.shape, 0)
        rank = kept_rank(token, w, patch_counts, placement)
        compact[...] = jnp.where(slot == rank, 1.0, 0.0).astype(jnp.bfloat16)

        def one(step, carry):
            text_load(raw, step).wait()
            texts[t, step] = jnp.dot(compact[...], raw[step], preferred_element_type=jnp.float32).astype(jnp.bfloat16)

            @pl.when(step < 4)
            def _():
                line_own(step)

            return carry

        lax.fori_loop(0, STEPS, one, 0)

    pl.run_scoped(
        compact_text,
        pltpu.VMEM((STEPS, text.shape[0], depth), jnp.bfloat16),
    )

    def open_weights(step, carry):
        for load in weight_loads(step):
            load.wait()
        send(X_OWN, step)
        send(CORE_OWN, step)
        return carry

    lax.fori_loop(0, STEPS, open_weights, 0)

    def attend(qkv_held, proj_held):
        loads = [
            pltpu.make_async_copy(vit_qkv, qkv_held, load_sem.at[1]),
            pltpu.make_async_copy(vit_proj, proj_held, load_sem.at[2]),
        ]
        for load in loads:
            load.start()
        up_load.start()
        normed = layer_norm(patches[...].astype(jnp.float32), vit_gain[...].reshape(1, -1)).astype(jnp.bfloat16)
        loads[0].wait()
        queries, keys, values = [
            lax.dot_general(
                normed, qkv_held[entry], (((1,), (1,)), ((), ())), preferred_element_type=jnp.float32
            )
            for entry in range(3)
        ]
        keys = keys.astype(jnp.bfloat16)
        count = patches.shape[0]
        row = lax.broadcasted_iota(jnp.int32, (count, count), 0) // MAXP
        column = lax.broadcasted_iota(jnp.int32, (count, count), 1) // MAXP
        index = lax.broadcasted_iota(jnp.int32, (1, count), 1)
        limit = jnp.zeros((1, count), jnp.int32)
        for image in range(IMG_DEV):
            limit = jnp.where(index // MAXP == image, image * MAXP + patch_counts[w * IMG_DEV + image], limit)
        seen = (row == column) & (index < limit)
        lane = lax.broadcasted_iota(jnp.int32, queries.shape, 1) // VHD
        context = jnp.zeros(queries.shape, jnp.float32)
        for head in range(queries.shape[1] // VHD):
            own = lane == head
            scores = lax.dot_general(
                jnp.where(own, queries, 0.0).astype(jnp.bfloat16),
                keys,
                (((1,), (1,)), ((), ())),
                preferred_element_type=jnp.float32,
            ) * VHD ** (-0.5)
            scores = jnp.where(seen, scores, -jnp.inf)
            raised = jnp.exp(scores - jnp.max(scores, axis=-1, keepdims=True))
            probs = (raised / jnp.sum(raised, axis=-1, keepdims=True)).astype(jnp.bfloat16)
            context = context + jnp.dot(
                probs, jnp.where(own, values, 0.0).astype(jnp.bfloat16), preferred_element_type=jnp.float32
            )
        loads[1].wait()
        part[...] = jnp.dot(
            context.astype(jnp.bfloat16), proj_held[...], preferred_element_type=jnp.float32
        ).astype(jnp.bfloat16)

    pl.run_scoped(attend, pltpu.VMEM(vit_qkv.shape, jnp.bfloat16), pltpu.VMEM(vit_proj.shape, jnp.bfloat16))

    own_rows = part.shape[0] // ring

    def share_piece(member):
        return part.at[pl.ds(pl.multiple_of(member * own_rows, own_rows), own_rows)]

    hand_in, swap, hand_back, result, finish_shares = scatter(
        0, share_piece, shares_relay, shares_crossed, shares_sum, shares_in
    )
    hand_in()
    line_own(4)
    line_pass(1, 0)
    swap()
    line_pass(1, 1)
    line_pass(2, 0)
    hand_back()
    line_own(5)
    line_pass(1, 2)
    for step in range(3):
        pass_on(step)
    total[...] = jnp.zeros_like(total)
    squares[...] = jnp.zeros_like(squares)
    handoff_masks(w, wide, visuals.shape[2], patch_counts, placement, pick, place, place_rows)
    token = lax.broadcasted_iota(jnp.int32, (expand.shape[0], 1), 0)
    slot = lax.broadcasted_iota(jnp.int32, expand.shape, 1)
    rank = kept_rank(token, w, patch_counts, placement)
    expand[...] = jnp.where(slot == rank, 1.0, 0.0).astype(jnp.bfloat16)
    rotary_tables(positions, inverse, (compact, place_rows), cosine, sine)

    own_patches = patches[pl.ds(pl.multiple_of(t * own_rows, own_rows), own_rows)]
    mixed = own_patches.astype(jnp.float32) + result()
    normed = layer_norm(mixed, merger_gain[...].reshape(1, -1)).astype(jnp.bfloat16)
    joined = merged.shape[0]
    chosen = (own_rows // joined, own_rows)
    row, column = lax.broadcasted_iota(jnp.int32, chosen, 0), lax.broadcasted_iota(jnp.int32, chosen, 1)
    for entry in range(joined):
        picks = (column == row * joined + entry).astype(jnp.float32).astype(jnp.bfloat16)
        merged[entry, t] = jnp.dot(picks, normed, preferred_element_type=jnp.float32).astype(jnp.bfloat16)
    out, arrive, finish_merged = gather(6, lambda member: merged.at[:, member])
    out()
    line_pass(2, 1)
    line_own(6)
    line_pass(1, 3)
    for step in range(3, 5):
        pass_on(step)
    for step in range(2):
        pass_core(step)
    arrive()

    up_load.wait()
    rows = own_rows // joined * ring
    inner = merged.shape[-1]
    raised = None
    for entry in range(joined):
        term = jnp.dot(
            merged[entry].reshape(rows, inner),
            up_held[pl.ds(entry * inner, inner)],
            preferred_element_type=jnp.float32,
        )
        raised = term if raised is None else raised + term
    hidden[...] = (0.5 * raised * (1.0 + lax.erf(raised * 0.5**0.5))).astype(jnp.bfloat16)

    features = visuals.shape[-1]
    tile = features // 4
    hand_in, swap, hand_back, result, finish_visual = scatter(
        9, lambda member: visual_part.at[member], visual_relay, visual_crossed, visual_sum, visual_in
    )

    def project_down(down_held):
        def load(member, slot):
            columns = pl.ds(pl.multiple_of(member * features, features), features)
            return pltpu.make_async_copy(merger_down.at[:, columns], down_held.at[slot], load_sem.at[3 + slot])

        def make(member, slot):
            load(member, slot).wait()

            def column(entry, carry):
                columns = pl.ds(pl.multiple_of(entry * tile, tile), tile)
                visual_part[member, :, columns] = jnp.dot(
                    hidden[...], down_held[slot, :, columns], preferred_element_type=jnp.float32
                ).astype(jnp.bfloat16)
                return carry

            lax.fori_loop(0, features // tile, column, 0)

        order = (half_start, half_start + 1, near, t)
        load(order[0], 0).start()
        load(order[1], 1).start()
        make(order[0], 0)
        load(order[2], 0).start()
        make(order[1], 1)
        load(order[3], 1).start()
        make(order[2], 0)
        hand_in()
        make(order[3], 1)

    pl.run_scoped(project_down, pltpu.VMEM((2, merger_down.shape[0], features), jnp.bfloat16))
    line_pass(2, 2)
    line_own(7)
    line_pass(1, 4)
    for step in range(5, 7):
        pass_on(step)
    for step in range(2, 4):
        pass_core(step)
    swap()
    line_pass(2, 3)
    hand_back()
    line_pass(1, 5)
    for step in range(7, STEPS):
        pass_on(step)

    picked = result().astype(jnp.bfloat16)
    packed[...] = (
        jnp.dot(pick[...], picked, preferred_element_type=jnp.float32)
        .astype(jnp.bfloat16)
        .reshape(packed.shape)
    )
    visuals[t, w] = packed[w]
    hand = [
        remote(packed.at[owner], visuals.at[t, w], side_send.at[15 + entry], side_recv.at[15 + entry], {"wide": owner})
        for entry, owner in enumerate((core, across, diagonal))
    ]
    for copy in hand:
        copy.start()
    line_pass(2, 4)
    for step in range(4, 6):
        pass_core(step)
    for entry, owner in enumerate((core, across, diagonal)):
        block = visuals.at[t, owner]
        remote(block, block, side_send.at[15 + entry], side_recv.at[15 + entry], {"wide": owner}).wait_recv()
    out, arrive, finish_rows = gather(18, lambda member: visuals.at[member])
    out()
    line_pass(1, 6)
    for step in range(6, STEPS):
        pass_core(step)
    line_pass(2, 5)
    arrive()
    line_pass(1, 7)

    kept, slots = texts.shape[2], total.shape[0] - texts.shape[2]
    upper = t // (ring // 2)

    def scale_rows(rows, values, columns, scale):
        lanes = squares.shape[1]
        folded = values * values
        for start in range(0, values.shape[1], lanes):
            squares[rows] += folded[:, start : start + lanes]
        scaled[rows, columns] = (values * scale).astype(jnp.bfloat16)

    def consume(step, groups):
        for kind in (CORE_OWN, CORE_X, CORE_Y):
            received(kind, step)
        columns = pl.ds(pl.multiple_of(step * depth, depth), depth)
        for group in groups:
            if group.stop == ring:
                line_received(ring - 2, step)
            for entry in group:
                block = entry + upper * (ring - 1 - 2 * entry)
                scale = gain[pl.ds(pl.multiple_of(block * features + step * depth, depth), depth)].reshape(1, -1)
                held = pl.ds(pl.multiple_of(block * depth, depth), depth)
                scale_rows(pl.ds(0, kept), texts[block, step].astype(jnp.float32), held, scale)
                brought = visuals[block, :, :, columns].reshape(slots, depth).astype(jnp.float32)
                scale_rows(pl.ds(kept, slots), brought, held, scale)
            first_block = 0 if len(group) == ring else upper if group.start == 0 else (1 - upper) * (ring - 1)
            span = pl.ds(pl.multiple_of(first_block * depth, depth), len(group) * depth)
            total[...] += jnp.dot(scaled[:, span], weights[step, span], preferred_element_type=jnp.float32)

    def consume_whole(step, carry):
        @pl.when(step < STEPS - 6)
        def _():
            line_pass(2, step + 6)

        consume(step, (range(ring),))
        return carry

    lax.fori_loop(0, STEPS - 1, consume_whole, 0)
    consume(STEPS - 1, (range(ring - 1), range(ring - 1, ring)))

    square = jnp.sum(squares[...], axis=1, keepdims=True) / gain.shape[0]
    squares[...] = jnp.broadcast_to(lax.rsqrt(square + NORM_EPS), squares.shape)

    def turned(start):
        values = total[:, pl.ds(start, HD)] * squares[...]
        return (values * cosine[...] + pltpu.roll(values, HD // 2, 1) * sine[...]).astype(jnp.bfloat16)

    def turned_head(entry, carry):
        start = pl.multiple_of(entry * HD, HD)
        rows_out[:, pl.ds(start, HD)] = turned(start)
        return carry

    lax.fori_loop(0, second // HD, turned_head, 0)
    for start in range(second, total.shape[1], HD):
        values = total[:, start : start + HD] * squares[...]
        rows_out[:, start : start + HD] = values.astype(jnp.bfloat16)

    def drain(step, carry):
        for kind in range(LINE):
            sent(kind, step)
        for hop in range(ring - 1):
            line_send(hop, step, lambda copy: copy.wait_send())
        return carry

    lax.fori_loop(0, STEPS, drain, 0)
    finish_shares()
    finish_merged()
    finish_visual()
    finish_rows()
    for copy in hand:
        copy.wait_send()


def kept_rank(token, owner, patch_counts, placement):
    rank, taken = token, jnp.zeros(token.shape, jnp.int32)
    for image in range(patch_counts.shape[0]):
        begin = placement[1, image]
        length = jnp.where(placement[0, image] == owner, patch_counts[image] // 4, 0)
        rank = rank - jnp.minimum(jnp.maximum(token - begin, 0), length)
        taken = jnp.where((token >= begin) & (token < begin + length), 1, taken)
    return jnp.where(taken == 1, -1, rank)


def place_results(rows, expand, place, *results):
    kept = expand.shape[1]
    start = 0
    for result in results:
        columns = pl.ds(start, result.shape[1])
        placed = jnp.dot(expand[...], rows[:kept, columns], preferred_element_type=jnp.float32)
        placed = placed + jnp.dot(place[...], rows[kept:, columns], preferred_element_type=jnp.float32)
        result[...] = placed.astype(result.dtype)
        start += result.shape[1]


def handoff_masks(owner, wide, capacity, patch_counts, placement, pick, place, place_rows):
    def grid(ref):
        return [lax.broadcasted_iota(jnp.int32, ref.shape, axis) for axis in range(2)]

    slot, row = grid(pick)
    views = (grid(place), grid(place_rows)[::-1])
    picked = jnp.zeros(pick.shape, jnp.float32)
    placed = [jnp.zeros(ref.shape, jnp.float32) for ref in (place, place_rows)]
    for source in range(wide):
        images = [source * IMG_DEV + entry for entry in range(IMG_DEV)]
        owners = [placement[0, image] for image in images]
        counts = [patch_counts[image] // 4 for image in images]
        mine = jnp.where(owner == source, 1, 0)
        for entry, image in enumerate(images):
            offset = 0
            for earlier in range(entry):
                offset = offset + jnp.where(owners[earlier] == owners[entry], counts[earlier], 0)
            start = owners[entry] * capacity + offset
            live = (slot >= start) & (slot < start + counts[entry] * mine)
            picked = jnp.where(live & (row - slot == entry * MAXM - start), 1.0, picked)
            begin = placement[1, image]
            length = jnp.where(owners[entry] == owner, counts[entry], 0)
            for entry_view, (token, place_slot) in enumerate(views):
                inside = (token >= begin) & (token < begin + length)
                match = inside & (place_slot - token == source * capacity + offset - begin)
                placed[entry_view] = jnp.where(match, 1.0, placed[entry_view])
    pick[...] = picked.astype(pick.dtype)
    place[...] = placed[0].astype(place.dtype)
    place_rows[...] = placed[1].astype(place_rows.dtype)


def rotary_tables(positions, inverse, row_maps, cosine, sine):
    lane = lax.broadcasted_iota(jnp.int32, cosine.shape, 1)
    ordinal = lax.rem(lane, HD // 2)
    high = positions[...] // 128
    parts = [part.astype(jnp.float32) for part in (high, positions[...] - high * 128)]
    empty = jnp.zeros((2, parts[0].shape[1]), jnp.float32)
    parts = jnp.concatenate([*parts, empty], axis=0).T.astype(jnp.bfloat16)
    moved = jnp.concatenate(
        [jnp.dot(ref[...], parts, preferred_element_type=jnp.float32) for ref in row_maps], axis=0
    )
    wanted = moved[:, 0:3] * 128.0 + moved[:, 3:6]
    first_end = HD // 8
    second = first_end + 3 * HD // 16
    chosen = jnp.where(
        ordinal < first_end, wanted[:, 0:1], jnp.where(ordinal < second, wanted[:, 1:2], wanted[:, 2:3])
    )
    angles = chosen * inverse[...]
    cosine[...] = jnp.cos(angles)
    turned = jnp.sin(angles)
    sine[...] = jnp.where(lane < HD // 2, -turned, turned)


def per_device_kernel(
    patches,
    patch_counts,
    placement,
    positions,
    text_embeds,
    vit_gain,
    vit_qkv,
    vit_proj,
    merger_gain,
    merger_up,
    merger_down,
    llm_gain,
    llm_query,
    llm_key,
    llm_value,
):
    wide, ring = lax.axis_size("wide"), lax.axis_size("tp")
    capacity = MAXM * ((IMG_DEV + wide - 1) // wide)
    merged_rows = IMG_DEV * MAXM
    slots = wide * capacity
    frequency = jnp.arange(HD).astype(jnp.float32) % (HD // 2)
    inverse = (ROPE_BASE ** (-2.0 * frequency / HD)).reshape(1, HD)
    tokens, features = text_embeds.shape
    depth_all = llm_query.shape[0]
    columns = llm_query.shape[1] + llm_key.shape[1] + llm_value.shape[1]
    depth = depth_all // STEPS
    kept = tokens - IMG_DEV * LEAST_MERGED
    own_rows = patches.shape[0] // ring
    joined = merger_up.shape[0] // VD
    hidden_units = merger_up.shape[1]
    bf16, f32 = jnp.bfloat16, jnp.float32
    smem, vmem = pl.BlockSpec(memory_space=pltpu.SMEM), pl.BlockSpec(memory_space=pltpu.VMEM)
    anywhere = pl.BlockSpec(memory_space=pl.ANY)
    rows, expand, place = pl.pallas_call(
        prompt_kernel,
        out_shape=[
            jax.ShapeDtypeStruct((kept + slots, columns), bf16),
            jax.ShapeDtypeStruct((tokens, kept), bf16),
            jax.ShapeDtypeStruct((tokens, slots), bf16),
        ],
        in_specs=[smem] * 2 + [vmem] * 4 + [anywhere] * 2 + [vmem] + [anywhere] * 3 + [vmem] + [anywhere] * 3,
        out_specs=[vmem] * 3,
        scratch_shapes=[
            pltpu.VMEM((STEPS, wide * depth, columns), bf16),
            pltpu.VMEM((ring, STEPS, kept, depth), bf16),
            pltpu.VMEM((kept + slots, columns), f32),
            pltpu.VMEM((kept + slots, HD), f32),
            pltpu.VMEM((kept + slots, ring * depth), bf16),
            pltpu.VMEM((kept, tokens), bf16),
            pltpu.VMEM(merger_up.shape, bf16),
            pltpu.VMEM(patches.shape, bf16),
            pltpu.VMEM((2, own_rows, VD), bf16),
            pltpu.VMEM((2, own_rows, VD), bf16),
            pltpu.VMEM((3, own_rows, VD), bf16),
            pltpu.VMEM((own_rows, VD), bf16),
            pltpu.VMEM((joined, ring, own_rows // joined, VD), bf16),
            pltpu.VMEM((merged_rows, hidden_units), bf16),
            pltpu.VMEM((ring, merged_rows, features), bf16),
            pltpu.VMEM((2, merged_rows, features), bf16),
            pltpu.VMEM((2, merged_rows, features), bf16),
            pltpu.VMEM((3, merged_rows, features), bf16),
            pltpu.VMEM((merged_rows, features), bf16),
            pltpu.VMEM((wide, capacity, features), bf16),
            pltpu.VMEM((ring, wide, capacity, features), bf16),
            pltpu.VMEM((slots, merged_rows), bf16),
            pltpu.VMEM((slots, tokens), bf16),
            pltpu.VMEM((kept + slots, HD), f32),
            pltpu.VMEM((kept + slots, HD), f32),
            pltpu.SemaphoreType.DMA((4, STEPS)),
            pltpu.SemaphoreType.DMA((5,)),
            pltpu.SemaphoreType.DMA((LINE + 2 * (ring - 1), STEPS)),
            pltpu.SemaphoreType.DMA((LINE + 2 * (ring - 1), STEPS)),
            pltpu.SemaphoreType.DMA((18 + ring - 1,)),
            pltpu.SemaphoreType.DMA((18 + ring - 1,)),
        ],
        compiler_params=pltpu.CompilerParams(
            collective_id=0, has_side_effects=True, vmem_limit_bytes=67043328
        ),
    )(
        patch_counts,
        placement.T,
        inverse,
        positions,
        patches,
        vit_gain,
        jnp.transpose(vit_qkv, (1, 2, 0)),
        vit_proj,
        merger_gain,
        merger_up,
        merger_down,
        text_embeds,
        llm_gain,
        llm_query,
        llm_key,
        llm_value,
    )

    share = tokens // 2
    return pl.pallas_call(
        place_results,
        grid=(2,),
        out_shape=[
            jax.ShapeDtypeStruct((tokens, weight.shape[1]), bf16)
            for weight in (llm_query, llm_key, llm_value)
        ],
        in_specs=[
            pl.BlockSpec((kept + slots, columns), lambda step: (0, 0)),
            pl.BlockSpec((share, kept), lambda step: (step, 0)),
            pl.BlockSpec((share, slots), lambda step: (step, 0)),
        ],
        out_specs=[
            pl.BlockSpec((share, weight.shape[1]), lambda step: (step, 0))
            for weight in (llm_query, llm_key, llm_value)
        ],
    )(rows, expand, place)


def solution(mesh):
    ring = mesh.shape["tp"] == 4 and mesh.shape["wide"] == 4 and mesh.shape["groups"] == 2
    return jax.shard_map(
        per_device_kernel if ring else per_device_rings,
        mesh=mesh,
        in_specs=(
            P(("groups", "wide"), None),
            P("groups"),
            P("groups", None),
            P(None, ("groups", "wide")),
            P(("groups", "wide"), "tp"),
            P(),
            P(None, None, "tp"),
            P("tp", None),
            P(),
            P(None, "tp"),
            P("tp", None),
            P(),
            P("wide", "tp"),
            P("wide", "tp"),
            P("wide", "tp"),
        ),
        out_specs=(
            P(("groups", "wide"), "tp"),
            P(("groups", "wide"), "tp"),
            P(("groups", "wide"), "tp"),
        ),
        check_vma=False,
    )
```

```python
import jax
import jax.numpy as jnp
from jax import lax
from jax.experimental import pallas as pl
from jax.experimental.pallas import tpu as pltpu
from jax.sharding import PartitionSpec as P

VD = 1280
HD = 128
IMG_DEV = 8
MAXP = 32
TOK_DEV = 512
VHD = 80
MAXM = 8


NORM_EPS = 1e-06
ROPE_BASE = 1000000.0


def layer_norm(inputs, scale_gain):
    center = jnp.mean(inputs, axis=-1, keepdims=True)
    shifted = inputs - center
    spread = jnp.mean(shifted * shifted, axis=-1, keepdims=True)
    return shifted * lax.rsqrt(spread + NORM_EPS) * scale_gain


def rms_norm(inputs, scale_gain):
    square = jnp.mean(inputs * inputs, axis=-1, keepdims=True)
    return inputs * lax.rsqrt(square + NORM_EPS) * scale_gain


def rotary(values, positions):
    half_size = HD // 2
    frequency = jnp.arange(half_size).astype(jnp.float32)
    inverse = ROPE_BASE ** (-2.0 * frequency / HD)
    first_end = HD // 8
    second = first_end + 3 * HD // 16
    ordinal = jnp.arange(half_size)
    section = jnp.where(ordinal < first_end, 0, jnp.where(ordinal < second, 1, 2))
    chosen = jnp.where(
        section[:, None] == 0,
        positions[0][None, :],
        jnp.where(section[:, None] == 1, positions[1][None, :], positions[2][None, :]),
    )
    angles = chosen.T.astype(jnp.float32) * inverse[None, :]
    angles = jnp.concatenate([angles, angles], axis=1)
    cosine = jnp.cos(angles)[:, None, :]
    sine_table = jnp.sin(angles)[:, None, :]
    upper_half = values[..., :half_size]
    lower_half = values[..., half_size:]
    turned = jnp.concatenate([-lower_half, upper_half], axis=-1)
    return values * cosine + turned * sine_table


def handoff_tables(patch_counts, placement, width_wide, myself, capacity):
    merged_count = patch_counts // 4
    owners = placement[:, 0]
    starts = placement[:, 1]
    owner_grid = owners.reshape(width_wide, IMG_DEV)
    count_grid = merged_count.reshape(width_wide, IMG_DEV)
    ordinal = jnp.arange(IMG_DEV)
    before = ordinal[:, None] < ordinal[None, :]
    same_owner = owner_grid[:, :, None] == owner_grid[:, None, :]
    offsets = jnp.sum(jnp.where(same_owner & before[None], count_grid[:, :, None], 0), axis=1)
    mine_owner = lax.dynamic_index_in_dim(owner_grid, myself, 0, keepdims=False)
    mine_count = lax.dynamic_index_in_dim(count_grid, myself, 0, keepdims=False)
    mine_offset = lax.dynamic_index_in_dim(offsets, myself, 0, keepdims=False)
    target = jnp.arange(width_wide)[:, None, None]
    slot_index = jnp.arange(capacity)[None, :, None]
    matches = (
        (mine_owner[None, None, :] == target)
        & (slot_index >= mine_offset[None, None, :])
        & (slot_index < mine_offset[None, None, :] + mine_count[None, None, :])
    )
    source_row = ordinal[None, None, :] * MAXM + slot_index - mine_offset[None, None, :]
    send_index = jnp.sum(jnp.where(matches, source_row, 0), axis=-1)
    send_live = jnp.any(matches, axis=-1)
    row_place = jnp.arange(TOK_DEV)[:, None]
    inside = (
        (owners[None, :] == myself)
        & (row_place >= starts[None, :])
        & (row_place < starts[None, :] + merged_count[None, :])
    )
    image_source = jnp.arange(owners.shape[0]) // IMG_DEV
    flat_slot = (
        image_source[None, :] * capacity
        + offsets.reshape(-1)[None, :]
        + row_place
        - starts[None, :]
    )
    take_index = jnp.sum(jnp.where(inside, flat_slot, 0), axis=-1)
    take_live = jnp.any(inside, axis=-1)
    return (send_index, send_live, take_index, take_live)


def pack_rows(visual, send_index, send_live):
    picked = jnp.take(visual, send_index.reshape(-1), axis=0)
    picked = picked.reshape(send_index.shape + (visual.shape[1],))
    return jnp.where(send_live[..., None], picked, jnp.zeros((), visual.dtype))


def exchange_sum(partial, axis_name, split_axis):
    members = lax.axis_size(axis_name)
    shape = partial.shape
    cut = shape[:split_axis] + (members, shape[split_axis] // members) + shape[split_axis + 1 :]
    stacked = jnp.moveaxis(partial.reshape(cut), split_axis, 0)
    swapped = lax.all_to_all(stacked, axis_name, split_axis=0, concat_axis=0, tiled=True)
    return jnp.sum(swapped.astype(jnp.float32), axis=0)


def doubling_gather(block, axis_name):
    members = lax.axis_size(axis_name)
    held = {0: block}
    bits = []
    step = 1
    while step < members:
        bits.append(step)
        step *= 2
    for bit in bits[1:] + bits[:1]:
        pairs = [(source, source ^ bit) for source in range(members)]
        for entry in sorted(held):
            held[entry ^ bit] = lax.ppermute(held[entry], axis_name, pairs)
    return [held[entry] for entry in range(members)]


def ring_gather_columns(block, axis_name):
    members = lax.axis_size(axis_name)
    me = lax.axis_index(axis_name)
    width = block.shape[1]
    up = [(source, (source + 1) % members) for source in range(members)]
    down = [(source, (source - 1) % members) for source in range(members)]
    gathered = jnp.zeros((block.shape[0], width * members), block.dtype)
    pieces = [(0, 0, block)]
    forward, backward = block, block
    distance = 1
    while 2 * distance < members:
        forward = lax.ppermute(forward, axis_name, up)
        backward = lax.ppermute(backward, axis_name, down)
        pieces.append((members - distance, 0, forward))
        pieces.append((distance, 0, backward))
        distance += 1
    if 2 * distance == members:
        half = width // 2
        pieces.append((distance, 0, lax.ppermute(forward[:, :half], axis_name, up)))
        pieces.append((distance, half, lax.ppermute(backward[:, half:], axis_name, down)))
    for offset, inner, piece in pieces:
        column = lax.rem(me + offset, members) * width + inner
        gathered = lax.dynamic_update_slice(gathered, piece, (0, column))
    return gathered


def project(rows, weight_blocks, member):
    depth = weight_blocks[0].shape[0]
    total = None
    for entry, block in enumerate(weight_blocks):
        columns = lax.dynamic_slice_in_dim(rows, (member ^ entry) * depth, depth, 1)
        share = jnp.dot(columns, block, preferred_element_type=jnp.float32)
        total = share if total is None else total + share
    return total


def per_device_rings(
    patches,
    patch_counts,
    placement,
    positions,
    text_embeds,
    vit_gain,
    vit_qkv,
    vit_proj,
    merger_gain,
    merger_up,
    merger_down,
    llm_gain,
    llm_query,
    llm_key,
    llm_value,
):
    width_wide = lax.axis_size("wide")
    myself = lax.axis_index("wide")
    capacity = MAXM * ((IMG_DEV + width_wide - 1) // width_wide)
    local_heads = vit_qkv.shape[2] // VHD
    own_weights = jnp.concatenate([llm_query, llm_key, llm_value], axis=1)
    weight_blocks = doubling_gather(own_weights, "wide")
    text_rows = ring_gather_columns(text_embeds, "tp")
    members = lax.axis_size("tp")
    patch_rows = patches.astype(jnp.float32)
    normed = layer_norm(patch_rows, vit_gain).astype(jnp.bfloat16)
    triple = jnp.dot(normed, vit_qkv.reshape(VD, -1), preferred_element_type=jnp.float32).astype(
        jnp.bfloat16
    )
    triple = triple.reshape(IMG_DEV, MAXP, 3, local_heads, VHD)
    scores = jnp.einsum(
        "iqhd,ikhd->ihqk", triple[:, :, 0], triple[:, :, 1], preferred_element_type=jnp.float32
    ) * VHD ** (-0.5)
    own_counts = lax.dynamic_slice_in_dim(patch_counts, myself * IMG_DEV, IMG_DEV)
    present = jnp.arange(MAXP)[None, :] < own_counts[:, None]
    scores = jnp.where(present[:, None, None, :], scores, -jnp.inf)
    highest = jnp.max(scores, axis=-1, keepdims=True)
    raised = jnp.exp(scores - highest)
    attention_weights = (raised / jnp.sum(raised, axis=-1, keepdims=True)).astype(jnp.bfloat16)
    context = jnp.einsum(
        "ihqk,ikhd->iqhd", attention_weights, triple[:, :, 2], preferred_element_type=jnp.float32
    ).astype(jnp.bfloat16)
    context = context.reshape(IMG_DEV * MAXP, local_heads * VHD)
    partial_heads = jnp.dot(context, vit_proj, preferred_element_type=jnp.float32)
    attended = exchange_sum(partial_heads.astype(jnp.bfloat16), "tp", 0)
    own_rows = IMG_DEV * MAXP // members
    own_patches = lax.dynamic_slice_in_dim(patches, lax.axis_index("tp") * own_rows, own_rows, 0)
    mixed_rows = own_patches.astype(jnp.float32) + attended
    own_merged = layer_norm(mixed_rows, merger_gain).astype(jnp.bfloat16)
    own_merged = own_merged.reshape(own_rows * MAXM // MAXP, 4 * VD)
    merged_in = lax.all_gather(own_merged, "tp", axis=0, tiled=True)
    hidden = jax.nn.gelu(
        jnp.dot(merged_in, merger_up, preferred_element_type=jnp.float32), approximate=False
    ).astype(jnp.bfloat16)
    partial_visual = jnp.dot(hidden, merger_down, preferred_element_type=jnp.float32)
    send_index, send_live, take_index, take_live = handoff_tables(
        patch_counts, placement, width_wide, myself, capacity
    )
    visual = exchange_sum(partial_visual.astype(jnp.bfloat16), "tp", 1).astype(jnp.bfloat16)
    outgoing = pack_rows(visual, send_index, send_live)
    incoming = lax.all_to_all(outgoing, "wide", split_axis=0, concat_axis=0, tiled=True)
    incoming = incoming.reshape(-1, incoming.shape[-1])
    copies = jnp.broadcast_to(incoming[None], (members,) + incoming.shape)
    spread_rows = lax.all_to_all(copies, "tp", split_axis=0, concat_axis=0, tiled=True)
    visual_rows = jnp.swapaxes(spread_rows, 0, 1).reshape(incoming.shape[0], -1)
    normed_text = rms_norm(text_rows.astype(jnp.float32), llm_gain).astype(jnp.bfloat16)
    normed_visual = rms_norm(visual_rows.astype(jnp.float32), llm_gain).astype(jnp.bfloat16)
    projected_text = project(normed_text, weight_blocks, myself)
    projected_visual = project(normed_visual, weight_blocks, myself)
    placed = jnp.take(projected_visual, take_index, axis=0)
    projected = jnp.where(take_live[:, None], placed, projected_text)
    first = llm_query.shape[1]
    second = first + llm_key.shape[1]
    projected_query = projected[:, :first]
    projected_key = projected[:, first:second]
    projected_value = projected[:, second:]
    queries = (
        rotary(projected_query.reshape(TOK_DEV, -1, HD), positions)
        .astype(jnp.bfloat16)
        .reshape(TOK_DEV, -1)
    )
    key_rows = (
        rotary(projected_key.reshape(TOK_DEV, -1, HD), positions)
        .astype(jnp.bfloat16)
        .reshape(TOK_DEV, -1)
    )
    value_rows = projected_value.astype(jnp.bfloat16)
    return (queries, key_rows, value_rows)


STEPS = 8
LEAST_MERGED = 6
MESH = pl.DeviceIdType.MESH
X_OWN, Y_PASS, CORE_OWN, CORE_X, CORE_Y, LINE = range(6)


def prompt_kernel(
    patch_counts,
    placement,
    inverse,
    positions,
    patches,
    vit_gain,
    vit_qkv,
    vit_proj,
    merger_gain,
    merger_up,
    merger_down,
    text,
    gain,
    w_query,
    w_key,
    w_value,
    rows_out,
    expand,
    place,
    weights,
    texts,
    total,
    squares,
    scaled,
    compact,
    up_held,
    part,
    shares_relay,
    shares_crossed,
    shares_sum,
    shares_in,
    merged,
    hidden,
    visual_part,
    visual_relay,
    visual_crossed,
    visual_sum,
    visual_in,
    packed,
    visuals,
    pick,
    place_rows,
    cosine,
    sine,
    local_sem,
    load_sem,
    bulk_send,
    bulk_recv,
    side_send,
    side_recv,
):
    groups, wide, ring = lax.axis_size("groups"), lax.axis_size("wide"), lax.axis_size("tp")
    g, w, t = lax.axis_index("groups"), lax.axis_index("wide"), lax.axis_index("tp")
    core = w + 1 - 2 * lax.rem(w, 2)
    across = lax.rem(w + 2, wide)
    diagonal = across + 1 - 2 * lax.rem(across, 2)
    other = lax.rem(g + 1, groups)
    above, below = {"tp": lax.rem(t + 1, ring)}, {"tp": lax.rem(t + ring - 1, ring)}
    depth = weights.shape[1] // wide
    half = depth // groups
    first, second = w_query.shape[1], w_query.shape[1] + w_key.shape[1]
    line = [lax.rem(t + distance, ring) for distance in range(1, ring)]

    barrier = pltpu.get_barrier_semaphore()
    peers = [{"tp": member} for member in line]
    peers += [{"wide": core}, {"wide": across}, {"wide": diagonal}, {"groups": other}]
    for peer in peers:
        pl.semaphore_signal(barrier, inc=1, device_id=peer, device_id_type=MESH)
    pl.semaphore_wait(barrier, len(peers))

    def remote(source, target, send, recv, peer):
        return pltpu.make_async_remote_copy(
            src_ref=source,
            dst_ref=target,
            send_sem=send,
            recv_sem=recv,
            device_id=peer,
            device_id_type=MESH,
        )

    def in_place(kind, step, ref, peer):
        return remote(ref, ref, bulk_send.at[kind, step], bulk_recv.at[kind, step], peer)

    def rows_of(block, step, offset, count):
        start = pl.multiple_of(block * depth + offset, 16)
        return weights.at[step, pl.ds(start, count)]

    bulk = {
        X_OWN: (lambda s: rows_of(w, s, g * half, half), lambda s: rows_of(across, s, g * half, half), {"wide": across}),
        Y_PASS: (lambda s: rows_of(across, s, g * half, half), lambda s: rows_of(across, s, other * half, half), {"groups": other}),
        CORE_OWN: (lambda s: rows_of(w, s, 0, depth), lambda s: rows_of(core, s, 0, depth), {"wide": core}),
        CORE_X: (lambda s: rows_of(across, s, g * half, half), lambda s: rows_of(diagonal, s, g * half, half), {"wide": core}),
        CORE_Y: (lambda s: rows_of(across, s, other * half, half), lambda s: rows_of(diagonal, s, other * half, half), {"wide": core}),
    }

    def send(kind, step):
        in_place(kind, step, bulk[kind][0](step), bulk[kind][2]).start()

    def sent(kind, step):
        in_place(kind, step, bulk[kind][0](step), bulk[kind][2]).wait_send()

    def received(kind, step):
        in_place(kind, step, bulk[kind][1](step), bulk[kind][2]).wait_recv()

    def weight_loads(step):
        rows = pl.ds(pl.multiple_of(step * depth, depth), depth)
        return [
            pltpu.make_async_copy(
                ref.at[rows], rows_of(w, step, 0, depth).at[:, pl.ds(start, ref.shape[1])], local_sem.at[entry, step]
            )
            for entry, (ref, start) in enumerate(((w_query, 0), (w_key, first), (w_value, second)))
        ]

    def text_load(raw, step):
        columns = pl.ds(pl.multiple_of(step * depth, depth), depth)
        return pltpu.make_async_copy(text.at[:, columns], raw.at[step], local_sem.at[3, step])

    def up_copy(hop, step, block):
        return in_place(LINE + hop, step, texts.at[block, step], above)

    def down_copy(hop, step, block):
        return in_place(LINE + ring - 1 + hop, step, texts.at[block, step], below)

    def line_send(hop, step, act=lambda copy: copy.start()):
        @pl.when(t + 1 < ring)
        def _():
            @pl.when(t >= hop)
            def _():
                act(up_copy(hop, step, t - hop))

        @pl.when(t > 0)
        def _():
            @pl.when(t + hop < ring)
            def _():
                act(down_copy(hop, step, t + hop))

    def line_received(hop, step):
        @pl.when(t > hop)
        def _():
            up_copy(hop, step, t - 1 - hop).wait_recv()

        @pl.when(t + 1 + hop < ring)
        def _():
            down_copy(hop, step, t + 1 + hop).wait_recv()

    def line_own(step):
        line_send(0, step)

    def line_pass(hop, step):
        line_received(hop - 1, step)
        line_send(hop, step)

    def pass_on(step):
        received(X_OWN, step)
        send(Y_PASS, step)
        send(CORE_X, step)

    def pass_core(step):
        received(Y_PASS, step)
        send(CORE_Y, step)

    near = t + 1 - 2 * lax.rem(t, 2)
    beyond = ring - 1 - t
    half_start = ring // 2 * lax.rem(t // 2 + 1, 2)
    inner_member = lax.rem(t // 2 + t, 2) == 1
    outer_member = jnp.logical_not(inner_member)

    def scatter(slot, pieces, relay, crossed, summed, arrived):
        def copy(entry, source, target, member):
            return remote(source, target, side_send.at[slot + entry], side_recv.at[slot + entry], {"tp": member})

        def hand_in(act=lambda copied: copied.start()):
            @pl.when(outer_member)
            def _():
                for entry in range(2):
                    act(copy(entry, pieces(half_start + entry), relay.at[entry], near))
                act(copy(2, pieces(near), arrived, near))

        def swap():
            @pl.when(outer_member)
            def _():
                crossed[...] = jnp.zeros_like(crossed)

            @pl.when(inner_member)
            def _():
                for entry in range(2):
                    copy(entry, relay.at[entry], relay.at[entry], near).wait_recv()
                    added = relay[entry].astype(jnp.float32) + pieces(half_start + entry)[...].astype(jnp.float32)
                    summed[entry] = added.astype(summed.dtype)
                for entry in range(2):
                    copy(3 + entry, summed.at[entry], crossed.at[entry], beyond).start()

        def hand_back():
            @pl.when(inner_member)
            def _():
                for entry in range(2):
                    copy(3 + entry, crossed.at[entry], crossed.at[entry], beyond).wait_recv()
                added = crossed[lax.rem(near, 2)].astype(jnp.float32) + pieces(near)[...].astype(jnp.float32)
                summed[2] = added.astype(summed.dtype)
                copy(5, summed.at[2], arrived, near).start()

        def result():
            @pl.when(inner_member)
            def _():
                copy(2, arrived, arrived, near).wait_recv()

            @pl.when(outer_member)
            def _():
                copy(5, arrived, arrived, near).wait_recv()

            own = pieces(t)[...].astype(jnp.float32)
            return own + arrived[...].astype(jnp.float32) + crossed[lax.rem(t, 2)].astype(jnp.float32)

        def finish():
            hand_in(lambda copied: copied.wait_send())

            @pl.when(inner_member)
            def _():
                for entry in range(2):
                    copy(3 + entry, summed.at[entry], crossed.at[entry], beyond).wait_send()
                copy(5, summed.at[2], arrived, near).wait_send()

        return hand_in, swap, hand_back, result, finish

    def gather(slot, block):
        def copy(distance, member, peer):
            ref = block(member)
            return remote(ref, ref, side_send.at[slot + distance], side_recv.at[slot + distance], {"tp": peer})

        def out():
            for distance, member in enumerate(line):
                copy(distance, t, member).start()

        def arrive():
            for distance in range(ring - 1):
                source = lax.rem(t + ring - 1 - distance, ring)
                copy(distance, source, source).wait_recv()

        def finish():
            for distance, member in enumerate(line):
                copy(distance, t, member).wait_send()

        return out, arrive, finish

    up_load = pltpu.make_async_copy(merger_up, up_held, load_sem.at[0])
    for step in range(STEPS):
        for load in weight_loads(step):
            load.start()

    def compact_text(raw):
        for step in range(STEPS):
            text_load(raw, step).start()
        token = lax.broadcasted_iota(jnp.int32, (1, compact.shape[1]), 1)
        slot = lax.broadcasted_iota(jnp.int32, compact.shape, 0)
        rank = kept_rank(token, w, patch_counts, placement)
        compact[...] = jnp.where(slot == rank, 1.0, 0.0).astype(jnp.bfloat16)

        def one(step, carry):
            text_load(raw, step).wait()
            texts[t, step] = jnp.dot(compact[...], raw[step], preferred_element_type=jnp.float32).astype(jnp.bfloat16)

            @pl.when(step < 4)
            def _():
                line_own(step)

            return carry

        lax.fori_loop(0, STEPS, one, 0)

    pl.run_scoped(
        compact_text,
        pltpu.VMEM((STEPS, text.shape[0], depth), jnp.bfloat16),
    )

    def open_weights(step, carry):
        for load in weight_loads(step):
            load.wait()
        send(X_OWN, step)
        send(CORE_OWN, step)
        return carry

    lax.fori_loop(0, STEPS, open_weights, 0)

    def attend(qkv_held, proj_held):
        loads = [
            pltpu.make_async_copy(vit_qkv, qkv_held, load_sem.at[1]),
            pltpu.make_async_copy(vit_proj, proj_held, load_sem.at[2]),
        ]
        for load in loads:
            load.start()
        up_load.start()
        normed = layer_norm(patches[...].astype(jnp.float32), vit_gain[...].reshape(1, -1)).astype(jnp.bfloat16)
        loads[0].wait()
        queries, keys, values = [
            lax.dot_general(
                normed, qkv_held[entry], (((1,), (1,)), ((), ())), preferred_element_type=jnp.float32
            )
            for entry in range(3)
        ]
        keys = keys.astype(jnp.bfloat16)
        count = patches.shape[0]
        row = lax.broadcasted_iota(jnp.int32, (count, count), 0) // MAXP
        column = lax.broadcasted_iota(jnp.int32, (count, count), 1) // MAXP
        index = lax.broadcasted_iota(jnp.int32, (1, count), 1)
        limit = jnp.zeros((1, count), jnp.int32)
        for image in range(IMG_DEV):
            limit = jnp.where(index // MAXP == image, image * MAXP + patch_counts[w * IMG_DEV + image], limit)
        seen = (row == column) & (index < limit)
        lane = lax.broadcasted_iota(jnp.int32, queries.shape, 1) // VHD
        context = jnp.zeros(queries.shape, jnp.float32)
        for head in range(queries.shape[1] // VHD):
            own = lane == head
            scores = lax.dot_general(
                jnp.where(own, queries, 0.0).astype(jnp.bfloat16),
                keys,
                (((1,), (1,)), ((), ())),
                preferred_element_type=jnp.float32,
            ) * VHD ** (-0.5)
            scores = jnp.where(seen, scores, -jnp.inf)
            raised = jnp.exp(scores - jnp.max(scores, axis=-1, keepdims=True))
            probs = (raised / jnp.sum(raised, axis=-1, keepdims=True)).astype(jnp.bfloat16)
            context = context + jnp.dot(
                probs, jnp.where(own, values, 0.0).astype(jnp.bfloat16), preferred_element_type=jnp.float32
            )
        loads[1].wait()
        part[...] = jnp.dot(
            context.astype(jnp.bfloat16), proj_held[...], preferred_element_type=jnp.float32
        ).astype(jnp.bfloat16)

    pl.run_scoped(attend, pltpu.VMEM(vit_qkv.shape, jnp.bfloat16), pltpu.VMEM(vit_proj.shape, jnp.bfloat16))

    own_rows = part.shape[0] // ring

    def share_piece(member):
        return part.at[pl.ds(pl.multiple_of(member * own_rows, own_rows), own_rows)]

    hand_in, swap, hand_back, result, finish_shares = scatter(
        0, share_piece, shares_relay, shares_crossed, shares_sum, shares_in
    )
    hand_in()
    line_own(4)
    line_pass(1, 0)
    swap()
    line_pass(1, 1)
    line_pass(2, 0)
    hand_back()
    line_own(5)
    line_pass(1, 2)
    for step in range(3):
        pass_on(step)
    total[...] = jnp.zeros_like(total)
    squares[...] = jnp.zeros_like(squares)
    handoff_masks(w, wide, visuals.shape[2], patch_counts, placement, pick, place, place_rows)
    token = lax.broadcasted_iota(jnp.int32, (expand.shape[0], 1), 0)
    slot = lax.broadcasted_iota(jnp.int32, expand.shape, 1)
    rank = kept_rank(token, w, patch_counts, placement)
    expand[...] = jnp.where(slot == rank, 1.0, 0.0).astype(jnp.bfloat16)
    rotary_tables(positions, inverse, (compact, place_rows), cosine, sine)

    own_patches = patches[pl.ds(pl.multiple_of(t * own_rows, own_rows), own_rows)]
    mixed = own_patches.astype(jnp.float32) + result()
    normed = layer_norm(mixed, merger_gain[...].reshape(1, -1)).astype(jnp.bfloat16)
    joined = merged.shape[0]
    chosen = (own_rows // joined, own_rows)
    row, column = lax.broadcasted_iota(jnp.int32, chosen, 0), lax.broadcasted_iota(jnp.int32, chosen, 1)
    for entry in range(joined):
        picks = (column == row * joined + entry).astype(jnp.float32).astype(jnp.bfloat16)
        merged[entry, t] = jnp.dot(picks, normed, preferred_element_type=jnp.float32).astype(jnp.bfloat16)
    out, arrive, finish_merged = gather(6, lambda member: merged.at[:, member])
    out()
    line_pass(2, 1)
    line_own(6)
    line_pass(1, 3)
    for step in range(3, 5):
        pass_on(step)
    for step in range(2):
        pass_core(step)
    arrive()

    up_load.wait()
    rows = own_rows // joined * ring
    inner = merged.shape[-1]
    raised = None
    for entry in range(joined):
        term = jnp.dot(
            merged[entry].reshape(rows, inner),
            up_held[pl.ds(entry * inner, inner)],
            preferred_element_type=jnp.float32,
        )
        raised = term if raised is None else raised + term
    hidden[...] = (0.5 * raised * (1.0 + lax.erf(raised * 0.5**0.5))).astype(jnp.bfloat16)

    features = visuals.shape[-1]
    tile = features // 4
    hand_in, swap, hand_back, result, finish_visual = scatter(
        9, lambda member: visual_part.at[member], visual_relay, visual_crossed, visual_sum, visual_in
    )

    def project_down(down_held):
        def load(member, slot):
            columns = pl.ds(pl.multiple_of(member * features, features), features)
            return pltpu.make_async_copy(merger_down.at[:, columns], down_held.at[slot], load_sem.at[3 + slot])

        def make(member, slot):
            load(member, slot).wait()

            def column(entry, carry):
                columns = pl.ds(pl.multiple_of(entry * tile, tile), tile)
                visual_part[member, :, columns] = jnp.dot(
                    hidden[...], down_held[slot, :, columns], preferred_element_type=jnp.float32
                ).astype(jnp.bfloat16)
                return carry

            lax.fori_loop(0, features // tile, column, 0)

        order = (half_start, half_start + 1, near, t)
        load(order[0], 0).start()
        load(order[1], 1).start()
        make(order[0], 0)
        load(order[2], 0).start()
        make(order[1], 1)
        load(order[3], 1).start()
        make(order[2], 0)
        hand_in()
        make(order[3], 1)

    pl.run_scoped(project_down, pltpu.VMEM((2, merger_down.shape[0], features), jnp.bfloat16))
    line_pass(2, 2)
    line_own(7)
    line_pass(1, 4)
    for step in range(5, 7):
        pass_on(step)
    for step in range(2, 4):
        pass_core(step)
    swap()
    line_pass(2, 3)
    hand_back()
    line_pass(1, 5)
    for step in range(7, STEPS):
        pass_on(step)

    picked = result().astype(jnp.bfloat16)
    packed[...] = (
        jnp.dot(pick[...], picked, preferred_element_type=jnp.float32)
        .astype(jnp.bfloat16)
        .reshape(packed.shape)
    )
    visuals[t, w] = packed[w]
    hand = [
        remote(packed.at[owner], visuals.at[t, w], side_send.at[15 + entry], side_recv.at[15 + entry], {"wide": owner})
        for entry, owner in enumerate((core, across, diagonal))
    ]
    for copy in hand:
        copy.start()
    line_pass(2, 4)
    for step in range(4, 6):
        pass_core(step)
    for entry, owner in enumerate((core, across, diagonal)):
        block = visuals.at[t, owner]
        remote(block, block, side_send.at[15 + entry], side_recv.at[15 + entry], {"wide": owner}).wait_recv()
    kept, slots = texts.shape[2], total.shape[0] - texts.shape[2]
    upper = t // (ring // 2)

    def scale_rows(rows, values, columns, scale):
        lanes = squares.shape[1]
        folded = values * values
        for start in range(0, values.shape[1], lanes):
            squares[rows] += folded[:, start : start + lanes]
        scaled[rows, columns] = (values * scale).astype(jnp.bfloat16)

    whole, text_rows, visual_rows = (0, kept + slots), (0, kept), (kept, slots)

    def consume(step, groups, rows=whole):
        if rows is not visual_rows:
            for kind in (CORE_OWN, CORE_X, CORE_Y):
                received(kind, step)
        columns = pl.ds(pl.multiple_of(step * depth, depth), depth)
        for group in groups:
            if group.stop == ring and rows is not visual_rows:
                line_received(ring - 2, step)
            for entry in group:
                block = entry + upper * (ring - 1 - 2 * entry)
                scale = gain[pl.ds(pl.multiple_of(block * features + step * depth, depth), depth)].reshape(1, -1)
                held = pl.ds(pl.multiple_of(block * depth, depth), depth)
                if rows is not visual_rows:
                    scale_rows(pl.ds(0, kept), texts[block, step].astype(jnp.float32), held, scale)
                if rows is not text_rows:
                    brought = visuals[block, :, :, columns].reshape(slots, depth).astype(jnp.float32)
                    scale_rows(pl.ds(kept, slots), brought, held, scale)
            first_block = 0 if len(group) == ring else upper if group.start == 0 else (1 - upper) * (ring - 1)
            span = pl.ds(pl.multiple_of(first_block * depth, depth), len(group) * depth)
            picked_rows = pl.ds(*rows)
            total[picked_rows] += jnp.dot(
                scaled[picked_rows, span], weights[step, span], preferred_element_type=jnp.float32
            )

    out, arrive, finish_rows = gather(18, lambda member: visuals.at[member])
    out()
    line_pass(1, 6)
    for step in range(6, STEPS):
        pass_core(step)
    line_pass(2, 5)
    line_pass(1, 7)

    early = STEPS - 2

    def consume_text(step, carry):
        consume(step, (range(ring),), text_rows)
        return carry

    def consume_visual(step, carry):
        consume(step, (range(ring),), visual_rows)
        return carry

    def consume_whole(step, carry):
        consume(step, (range(ring),))
        return carry

    lax.fori_loop(0, early, consume_text, 0)
    line_pass(2, 6)
    arrive()
    line_pass(2, 7)
    lax.fori_loop(0, early, consume_visual, 0)
    lax.fori_loop(early, STEPS - 1, consume_whole, 0)
    consume(STEPS - 1, (range(ring - 1), range(ring - 1, ring)))

    square = jnp.sum(squares[...], axis=1, keepdims=True) / gain.shape[0]
    squares[...] = jnp.broadcast_to(lax.rsqrt(square + NORM_EPS), squares.shape)

    def turned(start):
        values = total[:, pl.ds(start, HD)] * squares[...]
        return (values * cosine[...] + pltpu.roll(values, HD // 2, 1) * sine[...]).astype(jnp.bfloat16)

    def turned_head(entry, carry):
        start = pl.multiple_of(entry * HD, HD)
        rows_out[:, pl.ds(start, HD)] = turned(start)
        return carry

    lax.fori_loop(0, second // HD, turned_head, 0)
    for start in range(second, total.shape[1], HD):
        values = total[:, start : start + HD] * squares[...]
        rows_out[:, start : start + HD] = values.astype(jnp.bfloat16)

    def drain(step, carry):
        for kind in range(LINE):
            sent(kind, step)
        for hop in range(ring - 1):
            line_send(hop, step, lambda copy: copy.wait_send())
        return carry

    lax.fori_loop(0, STEPS, drain, 0)
    finish_shares()
    finish_merged()
    finish_visual()
    finish_rows()
    for copy in hand:
        copy.wait_send()


def kept_rank(token, owner, patch_counts, placement):
    rank, taken = token, jnp.zeros(token.shape, jnp.int32)
    for image in range(patch_counts.shape[0]):
        begin = placement[1, image]
        length = jnp.where(placement[0, image] == owner, patch_counts[image] // 4, 0)
        rank = rank - jnp.minimum(jnp.maximum(token - begin, 0), length)
        taken = jnp.where((token >= begin) & (token < begin + length), 1, taken)
    return jnp.where(taken == 1, -1, rank)


def place_results(rows, expand, place, *results):
    kept = expand.shape[1]
    start = 0
    for result in results:
        columns = pl.ds(start, result.shape[1])
        placed = jnp.dot(expand[...], rows[:kept, columns], preferred_element_type=jnp.float32)
        placed = placed + jnp.dot(place[...], rows[kept:, columns], preferred_element_type=jnp.float32)
        result[...] = placed.astype(result.dtype)
        start += result.shape[1]


def handoff_masks(owner, wide, capacity, patch_counts, placement, pick, place, place_rows):
    def grid(ref):
        return [lax.broadcasted_iota(jnp.int32, ref.shape, axis) for axis in range(2)]

    slot, row = grid(pick)
    views = (grid(place), grid(place_rows)[::-1])
    picked = jnp.zeros(pick.shape, jnp.float32)
    placed = [jnp.zeros(ref.shape, jnp.float32) for ref in (place, place_rows)]
    for source in range(wide):
        images = [source * IMG_DEV + entry for entry in range(IMG_DEV)]
        owners = [placement[0, image] for image in images]
        counts = [patch_counts[image] // 4 for image in images]
        mine = jnp.where(owner == source, 1, 0)
        for entry, image in enumerate(images):
            offset = 0
            for earlier in range(entry):
                offset = offset + jnp.where(owners[earlier] == owners[entry], counts[earlier], 0)
            start = owners[entry] * capacity + offset
            live = (slot >= start) & (slot < start + counts[entry] * mine)
            picked = jnp.where(live & (row - slot == entry * MAXM - start), 1.0, picked)
            begin = placement[1, image]
            length = jnp.where(owners[entry] == owner, counts[entry], 0)
            for entry_view, (token, place_slot) in enumerate(views):
                inside = (token >= begin) & (token < begin + length)
                match = inside & (place_slot - token == source * capacity + offset - begin)
                placed[entry_view] = jnp.where(match, 1.0, placed[entry_view])
    pick[...] = picked.astype(pick.dtype)
    place[...] = placed[0].astype(place.dtype)
    place_rows[...] = placed[1].astype(place_rows.dtype)


def rotary_tables(positions, inverse, row_maps, cosine, sine):
    lane = lax.broadcasted_iota(jnp.int32, cosine.shape, 1)
    ordinal = lax.rem(lane, HD // 2)
    high = positions[...] // 128
    parts = [part.astype(jnp.float32) for part in (high, positions[...] - high * 128)]
    empty = jnp.zeros((2, parts[0].shape[1]), jnp.float32)
    parts = jnp.concatenate([*parts, empty], axis=0).T.astype(jnp.bfloat16)
    moved = jnp.concatenate(
        [jnp.dot(ref[...], parts, preferred_element_type=jnp.float32) for ref in row_maps], axis=0
    )
    wanted = moved[:, 0:3] * 128.0 + moved[:, 3:6]
    first_end = HD // 8
    second = first_end + 3 * HD // 16
    chosen = jnp.where(
        ordinal < first_end, wanted[:, 0:1], jnp.where(ordinal < second, wanted[:, 1:2], wanted[:, 2:3])
    )
    angles = chosen * inverse[...]
    cosine[...] = jnp.cos(angles)
    turned = jnp.sin(angles)
    sine[...] = jnp.where(lane < HD // 2, -turned, turned)


def per_device_kernel(
    patches,
    patch_counts,
    placement,
    positions,
    text_embeds,
    vit_gain,
    vit_qkv,
    vit_proj,
    merger_gain,
    merger_up,
    merger_down,
    llm_gain,
    llm_query,
    llm_key,
    llm_value,
):
    wide, ring = lax.axis_size("wide"), lax.axis_size("tp")
    capacity = MAXM * ((IMG_DEV + wide - 1) // wide)
    merged_rows = IMG_DEV * MAXM
    slots = wide * capacity
    frequency = jnp.arange(HD).astype(jnp.float32) % (HD // 2)
    inverse = (ROPE_BASE ** (-2.0 * frequency / HD)).reshape(1, HD)
    tokens, features = text_embeds.shape
    depth_all = llm_query.shape[0]
    columns = llm_query.shape[1] + llm_key.shape[1] + llm_value.shape[1]
    depth = depth_all // STEPS
    kept = tokens - IMG_DEV * LEAST_MERGED
    own_rows = patches.shape[0] // ring
    joined = merger_up.shape[0] // VD
    hidden_units = merger_up.shape[1]
    bf16, f32 = jnp.bfloat16, jnp.float32
    smem, vmem = pl.BlockSpec(memory_space=pltpu.SMEM), pl.BlockSpec(memory_space=pltpu.VMEM)
    anywhere = pl.BlockSpec(memory_space=pl.ANY)
    rows, expand, place = pl.pallas_call(
        prompt_kernel,
        out_shape=[
            jax.ShapeDtypeStruct((kept + slots, columns), bf16),
            jax.ShapeDtypeStruct((tokens, kept), bf16),
            jax.ShapeDtypeStruct((tokens, slots), bf16),
        ],
        in_specs=[smem] * 2 + [vmem] * 4 + [anywhere] * 2 + [vmem] + [anywhere] * 3 + [vmem] + [anywhere] * 3,
        out_specs=[vmem] * 3,
        scratch_shapes=[
            pltpu.VMEM((STEPS, wide * depth, columns), bf16),
            pltpu.VMEM((ring, STEPS, kept, depth), bf16),
            pltpu.VMEM((kept + slots, columns), f32),
            pltpu.VMEM((kept + slots, HD), f32),
            pltpu.VMEM((kept + slots, ring * depth), bf16),
            pltpu.VMEM((kept, tokens), bf16),
            pltpu.VMEM(merger_up.shape, bf16),
            pltpu.VMEM(patches.shape, bf16),
            pltpu.VMEM((2, own_rows, VD), bf16),
            pltpu.VMEM((2, own_rows, VD), bf16),
            pltpu.VMEM((3, own_rows, VD), bf16),
            pltpu.VMEM((own_rows, VD), bf16),
            pltpu.VMEM((joined, ring, own_rows // joined, VD), bf16),
            pltpu.VMEM((merged_rows, hidden_units), bf16),
            pltpu.VMEM((ring, merged_rows, features), bf16),
            pltpu.VMEM((2, merged_rows, features), bf16),
            pltpu.VMEM((2, merged_rows, features), bf16),
            pltpu.VMEM((3, merged_rows, features), bf16),
            pltpu.VMEM((merged_rows, features), bf16),
            pltpu.VMEM((wide, capacity, features), bf16),
            pltpu.VMEM((ring, wide, capacity, features), bf16),
            pltpu.VMEM((slots, merged_rows), bf16),
            pltpu.VMEM((slots, tokens), bf16),
            pltpu.VMEM((kept + slots, HD), f32),
            pltpu.VMEM((kept + slots, HD), f32),
            pltpu.SemaphoreType.DMA((4, STEPS)),
            pltpu.SemaphoreType.DMA((5,)),
            pltpu.SemaphoreType.DMA((LINE + 2 * (ring - 1), STEPS)),
            pltpu.SemaphoreType.DMA((LINE + 2 * (ring - 1), STEPS)),
            pltpu.SemaphoreType.DMA((18 + ring - 1,)),
            pltpu.SemaphoreType.DMA((18 + ring - 1,)),
        ],
        compiler_params=pltpu.CompilerParams(
            collective_id=0, has_side_effects=True, vmem_limit_bytes=67043328
        ),
    )(
        patch_counts,
        placement.T,
        inverse,
        positions,
        patches,
        vit_gain,
        jnp.transpose(vit_qkv, (1, 2, 0)),
        vit_proj,
        merger_gain,
        merger_up,
        merger_down,
        text_embeds,
        llm_gain,
        llm_query,
        llm_key,
        llm_value,
    )

    share = tokens // 2
    return pl.pallas_call(
        place_results,
        grid=(2,),
        out_shape=[
            jax.ShapeDtypeStruct((tokens, weight.shape[1]), bf16)
            for weight in (llm_query, llm_key, llm_value)
        ],
        in_specs=[
            pl.BlockSpec((kept + slots, columns), lambda step: (0, 0)),
            pl.BlockSpec((share, kept), lambda step: (step, 0)),
            pl.BlockSpec((share, slots), lambda step: (step, 0)),
        ],
        out_specs=[
            pl.BlockSpec((share, weight.shape[1]), lambda step: (step, 0))
            for weight in (llm_query, llm_key, llm_value)
        ],
    )(rows, expand, place)


def solution(mesh):
    ring = mesh.shape["tp"] == 4 and mesh.shape["wide"] == 4 and mesh.shape["groups"] == 2
    return jax.shard_map(
        per_device_kernel if ring else per_device_rings,
        mesh=mesh,
        in_specs=(
            P(("groups", "wide"), None),
            P("groups"),
            P("groups", None),
            P(None, ("groups", "wide")),
            P(("groups", "wide"), "tp"),
            P(),
            P(None, None, "tp"),
            P("tp", None),
            P(),
            P(None, "tp"),
            P("tp", None),
            P(),
            P("wide", "tp"),
            P("wide", "tp"),
            P("wide", "tp"),
        ),
        out_specs=(
            P(("groups", "wide"), "tp"),
            P(("groups", "wide"), "tp"),
            P(("groups", "wide"), "tp"),
        ),
        check_vma=False,
    )
```
